128 devices in a mesh: seq: 64 (over z, y_lo, x, core), head: 2 (over y_hi).
Axes of the slice: x: 4, y: 4 (y_hi: 2, y_lo: 2; y = y_hi * 2 + y_lo), z: 4, core: 2. Of those that a mesh axis runs over, the one named last changes fastest.
Arguments:
- tokens: bfloat16 [32768, 4096], P('seq'), may hold values from -18 to 18
- norm_gain: float32 [4096], replicated, may hold values from 0.5 to 1.5
- w_query: bfloat16 [4096, 2048], P(None, 'head'), may hold values from -0.0625 to 0.0625
- w_key: bfloat16 [4096, 512], P(None, 'head'), may hold values from -1.90625 to 1.90625
- w_value: bfloat16 [4096, 512], P(None, 'head'), may hold values from -0.09375 to 0.09375
- w_out: bfloat16 [2048, 4096], P('head'), may hold values from -0.125 to 0.125
- window: int32 [16], P('head'), may hold values from 256 to 4096, as said below
- sink_count: int32 [16], P('head'), may hold values from 1 to 4, as said below
- sink_bias: float32 [16], P('head'), may hold values from 4 to 8
Outputs:
- mixed: bfloat16 [32768, 4096], P('seq', 'head')
The draws below stay inside these ranges and needn't reach their ends.
Inputs may be any that keep to these rules, and one draw needn't show every extreme that they name: Some head's window is exactly 4096. `sink_count`: some head's count is exactly 4.
All inputs are finite; a program needn't handle non-finite values.
Results may differ from the reference program's by a relative error of at most 0.0071.
Values may be sent and summed in bfloat16 or wider, within the bound.
A program may use at most 128 MiB of HBM per device.

```python
import jax
import jax.numpy as jnp
from jax import lax

D = 4096
HEADS = 16
KV_HEADS = 4
HEAD_DIM = 128
SINK = 4
WINMAX = 4096
T_DEV = 512
SPAN = 9
TOKENS = 32768
N_SEQ = 64
N_HEAD = 2


def query_matrix(key):
    base = jax.random.normal(jax.random.fold_in(key, 11), (D, HEADS * HEAD_DIM), jnp.float32)
    return jnp.clip(base, -4.0, 4.0) * D ** (-0.5)


def draw_w_query(key, part):
    return query_matrix(key).astype(jnp.bfloat16)


def draw_w_key(key, part):
    noise = jnp.clip(jax.random.normal(jax.random.fold_in(key, 12), (D, KV_HEADS, HEAD_DIM), jnp.float32), -4.0, 4.0) * D ** (-0.5)
    result = noise
    return result.reshape(D, KV_HEADS * HEAD_DIM).astype(jnp.bfloat16)


def draw_tokens(key, part):
    shape = (TOKENS, D)
    base = jnp.clip(jax.random.normal(jax.random.fold_in(key, 24), shape, jnp.float32), -6.0, 6.0)
    return base.astype(jnp.bfloat16)


def draw_window(key, part):
    lengths = jax.random.randint(jax.random.fold_in(key, 31), (HEADS,), T_DEV // 2, WINMAX + 1, jnp.int32)
    chosen = jax.random.randint(jax.random.fold_in(key, 32), (), 0, HEADS, jnp.int32)
    return jnp.where(jnp.arange(HEADS, dtype=jnp.int32) == chosen, WINMAX, lengths).astype(jnp.int32)


def draw_sink_count(key, part):
    counts = jax.random.randint(jax.random.fold_in(key, 41), (HEADS,), 1, SINK + 1, jnp.int32)
    chosen = jax.random.randint(jax.random.fold_in(key, 42), (), 0, HEADS, jnp.int32)
    return jnp.where(jnp.arange(HEADS, dtype=jnp.int32) == chosen, SINK, counts).astype(jnp.int32)


def shard_levels(stream_key, shape, pieces, low, high):
    level, own = 1.0, jax.random.fold_in(stream_key, 6)
    for dim, shards_of in pieces:
        draws = jnp.exp(jax.random.uniform(jax.random.fold_in(own, dim), (shards_of,), jnp.float32, low / len(pieces), high / len(pieces)))
        level = level * jnp.repeat(draws, shape[dim] // shards_of).reshape([-1 if axis == dim else 1 for axis in range(len(shape))])
    return level


def gaussian(key, dims, scale, limit, cuts=(), held_as=jnp.bfloat16):
    values = scale * jax.random.normal(key, dims, jnp.float32)
    if cuts:
        values = values * shard_levels(key, dims, cuts, -0.22, 0.18)
    return jnp.clip(values, -limit, limit).astype(held_as)


def setup_inputs(seed: int = 0) -> dict:
    keys = jax.random.split(jax.random.key(seed), 10)
    tokens = draw_tokens(jax.random.fold_in(keys[9], 71), 0)
    norm_gain = jnp.clip(1.0 + 0.1 * jax.random.normal(keys[1], (D,), jnp.float32), 0.5, 1.5)
    w_query = draw_w_query(jax.random.fold_in(keys[9], 71), 0)
    w_key = draw_w_key(jax.random.fold_in(keys[9], 71), 0)
    w_value = gaussian(keys[4], (D, KV_HEADS * HEAD_DIM), D ** -0.5, 0.09375, ((1, 2),))
    w_out = gaussian(keys[5], (HEADS * HEAD_DIM, D), (HEADS * HEAD_DIM) ** -0.5, 0.125, ((0, 2),))
    window = draw_window(jax.random.fold_in(keys[9], 71), 0)
    sink_count = draw_sink_count(jax.random.fold_in(keys[9], 71), 0)
    sink_bias = jnp.clip(4.0 + 4.0 * jax.random.uniform(keys[8], (HEADS,), jnp.float32) ** shard_levels(keys[8], (HEADS,), ((0, 2),), -0.2, 0.2), 4.0, 8.0)
    return dict(tokens=tokens, norm_gain=norm_gain, w_query=w_query, w_key=w_key, w_value=w_value, w_out=w_out, window=window, sink_count=sink_count, sink_bias=sink_bias)


EPSILON = 1e-05

def normalize(tokens, norm_gain):
    widened = tokens.astype(jnp.float32)
    row_scale = lax.rsqrt(lax.optimization_barrier(jnp.mean(widened * widened, axis=1, keepdims=True)) + EPSILON)
    return (widened, (widened * row_scale * norm_gain).astype(jnp.bfloat16))

def attend(queries, block_keys, block_values, anchor_key_rows, anchor_value_rows, query_start, key_start, window, sink_count, sink_bias):
    tok_rows, heads_here, head_width = queries.shape
    key_rows, groups_here, _ = block_keys.shape
    per_group = heads_here // groups_here
    query_groups = queries.astype(jnp.float32).reshape(tok_rows, groups_here, per_group, head_width)
    softmax_scale = head_width ** (-0.5)
    scores = jnp.einsum('tgre,lge->grtl', query_groups, block_keys.astype(jnp.float32)) * softmax_scale
    anchor_score_rows = jnp.einsum('yxmo,kxo->xmyk', query_groups, anchor_key_rows.astype(jnp.float32)) * softmax_scale
    anchor_score_rows = anchor_score_rows + sink_bias.reshape(groups_here, per_group)[:, :, None, None]
    query_pos = (query_start + jnp.arange(tok_rows, dtype=jnp.int32))[None, None, :, None]
    key_pos = (key_start + jnp.arange(key_rows, dtype=jnp.int32))[None, None, None, :]
    sink_pos = jnp.arange(anchor_key_rows.shape[0], dtype=jnp.int32)[None, None, None, :]
    reach_rows = window.reshape(groups_here, per_group)[:, :, None, None]
    open_sinks = sink_count.reshape(groups_here, per_group)[:, :, None, None]
    visible = (key_pos <= query_pos) & (key_pos > query_pos - reach_rows) & (key_pos >= 0)
    sink_open = (sink_pos < open_sinks) & (sink_pos <= query_pos - reach_rows)
    scores = jnp.where(visible, scores, -1e+30)
    anchor_score_rows = jnp.where(sink_open, anchor_score_rows, -1e+30)
    peak_score = jnp.maximum(lax.optimization_barrier(jnp.max(scores, axis=3, keepdims=True)), lax.optimization_barrier(jnp.max(anchor_score_rows, axis=3, keepdims=True)))
    weights = jnp.exp(scores - peak_score)
    anchor_weight_rows = jnp.exp(anchor_score_rows - peak_score)
    denominator = lax.optimization_barrier(jnp.sum(weights, axis=3, keepdims=True)) + lax.optimization_barrier(jnp.sum(anchor_weight_rows, axis=3, keepdims=True))
    weights = (weights / denominator).astype(jnp.bfloat16)
    anchor_weight_rows = (anchor_weight_rows / denominator).astype(jnp.bfloat16)
    merged_scores = jnp.einsum('grtl,lge->tgre', weights.astype(jnp.float32), block_values.astype(jnp.float32))
    merged_scores = merged_scores + jnp.einsum('pvlu,upc->lpvc', anchor_weight_rows.astype(jnp.float32), anchor_value_rows.astype(jnp.float32))
    return merged_scores.astype(jnp.bfloat16).reshape(tok_rows, heads_here * head_width)

def reference(tokens, norm_gain, w_query, w_key, w_value, w_out, window, sink_count, sink_bias):
    widened, normed = normalize(tokens, norm_gain)
    total_rows = tokens.shape[0]
    queries = jnp.dot(normed, w_query, preferred_element_type=jnp.float32).astype(jnp.bfloat16).reshape(total_rows, HEADS, HEAD_DIM)
    keys_all = jnp.dot(normed, w_key, preferred_element_type=jnp.float32).astype(jnp.bfloat16).reshape(total_rows, KV_HEADS, HEAD_DIM)
    values_all = jnp.dot(normed, w_value, preferred_element_type=jnp.float32).astype(jnp.bfloat16).reshape(total_rows, KV_HEADS, HEAD_DIM)
    margin = (SPAN - 1) * T_DEV
    padding = jnp.zeros((margin, KV_HEADS, HEAD_DIM), keys_all.dtype)
    padded_keys = jnp.concatenate([padding, keys_all], axis=0)
    padded_values = jnp.concatenate([padding, values_all], axis=0)
    anchor_key_rows = keys_all[:SINK]
    anchor_value_rows = values_all[:SINK]

    def one_block(block_index):
        query_start = (block_index * T_DEV).astype(jnp.int32)
        block_queries = lax.dynamic_slice_in_dim(queries, query_start, T_DEV, 0)
        block_keys = lax.dynamic_slice_in_dim(padded_keys, query_start, SPAN * T_DEV, 0)
        block_values = lax.dynamic_slice_in_dim(padded_values, query_start, SPAN * T_DEV, 0)
        return attend(block_queries, block_keys, block_values, anchor_key_rows, anchor_value_rows, query_start, query_start - margin, window, sink_count, sink_bias)
    attended = lax.map(one_block, jnp.arange(N_SEQ, dtype=jnp.int32)).reshape(total_rows, HEADS * HEAD_DIM)
    half_width = HEADS * HEAD_DIM // N_HEAD
    merged_scores = jnp.zeros((total_rows, D), jnp.float32)
    for part_index in range(N_HEAD):
        lower = part_index * half_width
        partial_term = jnp.dot(attended[:, lower:lower + half_width], w_out[lower:lower + half_width], preferred_element_type=jnp.float32).astype(jnp.bfloat16)
        merged_scores = merged_scores + lax.optimization_barrier(partial_term).astype(jnp.float32)
    return (widened + merged_scores).astype(jnp.bfloat16)
```

```python
import functools

import jax
import jax.numpy as jnp
from jax import lax
from jax.experimental import pallas as pl
from jax.experimental.pallas import tpu as pltpu
from jax.sharding import PartitionSpec as P

MESH = pl.DeviceIdType.MESH
HD = 128
T = 512
D = 4096
SINK = 4
SROWS = 16
EPS = 1e-05
LOG2E = 1.4426950408889634
CSCALE = LOG2E * HD ** (-0.5)
NEG = -1e30
F32 = jnp.float32
BF16 = jnp.bfloat16
QT = 256

S_PREV, S_POS, S_NEG, S_FPOS, S_FNEG, S_D2D = 0, 1, 2, 3, 4, 5
N_HALO_SEND = S_D2D + 5


def kernel(
    x_hbm, gain_ref, wq_hbm, wk_hbm, wv_hbm, wo_hbm, win_ref, cnt_ref, bias_ref,
    out_hbm,
    x_v, n_v, wq_v, wkv_v, wown_v, wpeer_v, kv_v, sink_v, q_v, acc_v, m_v, rel_v,
    att_v, attp_v, o0_v, o1_v, out_v,
    in_sem, hsend, hrecv, wsend, wrecv, ssend, srecv, asend, arecv, out_sem,
):
    seq = lax.axis_index("seq")
    j = lax.axis_index("head")
    k = seq % 2
    x = (seq // 2) % 4
    r = seq // 8
    yl = r % 2
    z = r // 2
    peer = 1 - j

    def at(z_, yl_, x_, k_):
        return ((z_ * 2 + yl_) * 4 + x_) * 2 + k_

    sib = (at(z, yl, x, 1 - k), j)
    rn = (r + 1) % 8
    next_row = (rn * 8 + x * 2 + k, j)
    xp = (at(z, yl, (x + 1) % 4, k), j)
    xm = (at(z, yl, (x + 3) % 4, k), j)
    x2 = (at(z, yl, (x + 2) % 4, k), j)
    zp = (at((z + 1) % 4, yl, x, k), j)
    zm = (at((z + 3) % 4, yl, x, k), j)
    yo = (at(z, 1 - yl, x, k), j)
    head_peer = (seq, peer)

    def rcopy(src, dst, ss, rs, dev):
        return pltpu.make_async_remote_copy(
            src_ref=src, dst_ref=dst, send_sem=ss, recv_sem=rs, device_id=dev, device_id_type=MESH
        )

    def xcopy(i):
        rows = pl.ds(i * 128, 128)
        return pltpu.make_async_copy(x_hbm.at[rows], x_v.at[rows], in_sem.at[i])

    def kvcopy(i):
        g, w = i // 2, i % 2
        src = wk_hbm if w == 0 else wv_hbm
        return pltpu.make_async_copy(
            src.at[:, pl.ds(g * HD, HD)], wkv_v.at[:, pl.ds(i * HD, HD)], in_sem.at[4 + i]
        )

    def qcopy(i):
        cols = pl.ds(i * 256, 256)
        return pltpu.make_async_copy(wq_hbm.at[:, cols], wq_v.at[:, cols], in_sem.at[8 + i])

    own_copy = pltpu.make_async_copy(
        wo_hbm.at[:, pl.ds(pl.multiple_of(j * 2048, 2048), 2048)], wown_v, in_sem.at[12]
    )
    L = ((k * 4 + z) * 4 + x) * 2 + yl
    w0 = rcopy(
        wo_hbm.at[pl.ds(L * 16, 16), pl.ds(pl.multiple_of(peer * 2048, 2048), 2048)],
        wpeer_v.at[L], wsend.at[0], wrecv.at[0], head_peer,
    )
    w0.start()
    for i in range(4):
        xcopy(i).start()
    for i in range(4):
        kvcopy(i).start()
    for i in range(4):
        qcopy(i).start()
    own_copy.start()

    w1 = rcopy(wpeer_v.at[L], wpeer_v.at[L], wsend.at[1], wrecv.at[1], yo)
    L2 = ((k * 4 + z) * 4 + x) * 2
    two = wpeer_v.at[pl.ds(L2, 2)]
    w2 = [rcopy(two, two, wsend.at[2 + i], wrecv.at[2 + i], d) for i, d in enumerate((xp, xm, x2))]
    L8 = (k * 4 + z) * 8
    eight = wpeer_v.at[pl.ds(L8, 8)]
    w3 = [rcopy(eight, eight, wsend.at[5 + i], wrecv.at[5 + i], d) for i, d in enumerate((zp, zm))]
    Lm = (k * 4 + (z + 3) % 4) * 8
    Lp = (k * 4 + (z + 1) % 4) * 8
    lo4 = wpeer_v.at[pl.ds(Lm, 4)]
    hi4 = wpeer_v.at[pl.ds(Lp + 4, 4)]
    w4 = [rcopy(lo4, lo4, wsend.at[7], wrecv.at[7], zp), rcopy(hi4, hi4, wsend.at[8], wrecv.at[8], zm)]
    half = wpeer_v.at[pl.ds(k * 32, 32)]
    w5 = rcopy(half, half, wsend.at[9], wrecv.at[9], sib)

    own_slot = k
    prev_slot = 8 + k

    def slot_copy(src_slot, dst_slot, g, srow, dev, rslot):
        return rcopy(kv_v.at[src_slot, g], kv_v.at[dst_slot, g], hsend.at[g, srow], hrecv.at[g, rslot], dev)

    def c_prev(g):
        return slot_copy(own_slot, 8 + k, g, S_PREV, next_row, 8 + k)

    def c_pos(g, src):
        return slot_copy(src, 2 + k, g, S_POS, xp, 2 + k)

    def c_neg(g, src):
        return slot_copy(src, 6 + k, g, S_NEG, xm, 6 + k)

    def c_fpos(g):
        return slot_copy(2 + k, 4 + k, g, S_FPOS, xp, 4 + k)

    def c_fneg(g):
        return slot_copy(6 + k, 4 + k, g, S_FNEG, xm, 4 + k)

    def c_d2d(g, d):
        return slot_copy(2 * d + k, 2 * d + k, g, S_D2D + d, sib, 2 * d + k)

    def wait_slot(g, s):
        slot_copy(s, s, g, S_PREV, sib, s).wait_recv()

    mid = (x == 1) | (x == 2)

    def start_own(g):
        c_prev(g).start()

        @pl.when(x < 3)
        def _():
            c_pos(g, own_slot).start()

        @pl.when(x == 0)
        def _():
            c_neg(g, own_slot).start()

        @pl.when(k == 0)
        def _():
            c_d2d(g, 0).start()

    def f_prev(g):
        wait_slot(g, 8 + k)

        @pl.when(x == 3)
        def _():
            c_pos(g, prev_slot).start()

        @pl.when(x > 0)
        def _():
            c_neg(g, prev_slot).start()

        @pl.when(k == 1)
        def _():
            c_d2d(g, 4).start()

    def f_one(g):
        wait_slot(g, 2 + k)

        @pl.when(mid)
        def _():
            c_fpos(g).start()

        c_d2d(g, 1).start()

    def f_three(g):
        wait_slot(g, 6 + k)

        @pl.when(mid)
        def _():
            c_fneg(g).start()

        c_d2d(g, 3).start()

    def f_two(g):
        wait_slot(g, 4 + k)
        c_d2d(g, 2).start()

    def wait_sends(g):
        c_prev(g).wait_send()
        c_pos(g, own_slot).wait_send()
        c_neg(g, own_slot).wait_send()

        @pl.when(mid)
        def _():
            c_fpos(g).wait_send()
            c_fneg(g).wait_send()

        @pl.when(k == 0)
        def _():
            c_d2d(g, 0).wait_send()

        @pl.when(k == 1)
        def _():
            c_d2d(g, 4).wait_send()

        for d in (1, 2, 3):
            c_d2d(g, d).wait_send()

    sinks = sink_v.at[:]
    s_x = [rcopy(sinks, sinks, ssend.at[i], srecv.at[0], (at(0, 0, i + 1, 0), j)) for i in range(3)]
    s_y = rcopy(sinks, sinks, ssend.at[3], srecv.at[1], yo)
    s_z = [rcopy(sinks, sinks, ssend.at[4 + i], srecv.at[2], (at(i + 1, yl, x, 0), j)) for i in range(3)]
    s_k = rcopy(sinks, sinks, ssend.at[7], srecv.at[3], sib)
    is_root = seq == 0
    tier_x = (z == 0) & (yl == 0) & (k == 0)
    tier_y = (z == 0) & (k == 0)
    tier_z = k == 0

    def rel_rows(i, c):
        rows = pl.ds(i * 64, 64)
        a = lax.broadcasted_iota(jnp.int32, (64, T), 0) + i * 64
        b = lax.broadcasted_iota(jnp.int32, (64, T), 1)
        rel_v[rows, :] = a - b
        return c

    lax.fori_loop(0, 8, rel_rows, 0)
    gain = gain_ref[...]

    def norm_rows(i, c):
        rows = pl.ds(i * 32, 32)
        xt = x_v[rows, :].astype(F32)
        ms = jnp.mean(xt * xt, axis=1, keepdims=True)
        n_v[rows, :] = (xt * lax.rsqrt(ms + EPS) * gain).astype(BF16)
        return c

    for i in range(4):
        xcopy(i).wait()
        lax.fori_loop(i * 4, i * 4 + 4, norm_rows, 0)

    w0.wait_recv()
    w1.start()

    for g in range(2):
        kvcopy(2 * g).wait()
        kvcopy(2 * g + 1).wait()
        y = jnp.dot(n_v[...], wkv_v[:, g * 256 : g * 256 + 256], preferred_element_type=F32)
        kv_v[own_slot, g] = y.astype(BF16)
        start_own(g)

    @pl.when(is_root)
    def _():
        for g in range(2):
            sink_v[g] = kv_v[0, g, :SROWS, :]
        for c in s_x:
            c.start()

    w1.wait_recv()
    for c in w2:
        c.start()

    def q_tile(i):
        qcopy(i).wait()
        y = jnp.dot(n_v[...], wq_v[:, i * 256 : i * 256 + 256], preferred_element_type=F32)
        for h in range(2):
            qs = y[:, h * HD : h * HD + HD].astype(BF16).astype(F32) * CSCALE
            hi = qs.astype(BF16)
            q_v[2 * i + h, :, 0:HD] = hi
            q_v[2 * i + h, :, HD : 2 * HD] = (qs - hi.astype(F32)).astype(BF16)

    q_tile(0)
    q_tile(1)

    @pl.when(tier_x)
    def _():
        @pl.when(jnp.logical_not(is_root))
        def _():
            s_x[0].wait_recv()

        s_y.start()

    q_tile(2)
    q_tile(3)
    for c in w2:
        c.wait_recv()
    for c in w3:
        c.start()

    ones = jnp.ones((T, HD), BF16)
    nt = (((1,), (1,)), ((), ()))

    def tile_step(g, idx, slots, first):
        h = g * 4 + idx // 2
        rows = pl.ds(pl.multiple_of((idx % 2) * QT, QT), QT)
        q = q_v[h, rows, :]
        rel = rel_v[rows, :]
        w = win_ref[h]
        parts = []
        top = None
        for d, kk in slots:
            dist = 2 * d + k - kk
            keys = kv_v[2 * d + kk, g, :, 0:HD]
            s = lax.dot_general(
                q, jnp.concatenate([keys, keys], axis=1), nt, preferred_element_type=F32
            )
            limit = jnp.where(seq >= dist, w - T * dist, -100000)
            seen = rel < limit
            if first:
                seen = seen & (rel >= 0)
            s = jnp.where(seen, s, NEG)
            parts.append(s)
            t = jnp.max(s, axis=1, keepdims=True)
            top = t if top is None else jnp.maximum(top, t)
        if not first:
            old = m_v[h, rows, 0:1]
            top = jnp.maximum(top, old)
        total = None
        for (d, kk), s in zip(slots, parts):
            p = jnp.exp2(s - top).astype(BF16)
            vals = kv_v[2 * d + kk, g, :, HD : 2 * HD]
            o = jnp.dot(p, jnp.concatenate([vals, ones], axis=1), preferred_element_type=F32)
            total = o if total is None else total + o
        if not first:
            total = total + acc_v[h, rows, :] * jnp.exp2(old - top)
        acc_v[h, rows, :] = total
        m_v[h, rows, :] = jnp.broadcast_to(top, (QT, HD))

    def step(g, slots, first=False):
        def body(idx, c):
            tile_step(g, idx, slots, first)
            return c

        lax.fori_loop(0, 8, body, 0)

    def finish_tile(g, idx):
        h = g * 4 + idx // 2
        rows = pl.ds(pl.multiple_of((idx % 2) * QT, QT), QT)
        q = q_v[h, rows, :]
        ks = sink_v[g, :, 0:HD]
        vs = sink_v[g, :, HD : 2 * HD]
        s = lax.dot_general(q, jnp.concatenate([ks, ks], axis=1), nt, preferred_element_type=F32)
        s = s + bias_ref[h] * LOG2E
        col = lax.broadcasted_iota(jnp.int32, (QT, SROWS), 1)
        pos = lax.broadcasted_iota(jnp.int32, (QT, SROWS), 0) + (seq * T + (idx % 2) * QT)
        is_open = (col < cnt_ref[h]) & (col < SINK) & (col <= pos - win_ref[h])
        s = jnp.where(is_open, s, NEG)
        old = m_v[h, rows, 0:1]
        top = jnp.maximum(jnp.max(s, axis=1, keepdims=True), old)
        p = jnp.exp2(s - top).astype(BF16)
        o = jnp.dot(
            p, jnp.concatenate([vs, jnp.ones((SROWS, HD), BF16)], axis=1), preferred_element_type=F32
        )
        o = o + acc_v[h, rows, :] * jnp.exp2(old - top)
        return rows, (o[:, 0:HD] / o[:, HD : 2 * HD]).astype(BF16)

    def c_att(pair):
        return rcopy(att_v.at[pair], attp_v.at[pair], asend.at[pair], arecv.at[pair], head_peer)

    def finish(g):
        for pair in range(2):
            for h in range(2):
                for t in range(2):
                    rows, val = finish_tile(g, (pair * 2 + h) * 2 + t)
                    att_v[g * 2 + pair, rows, h * HD : h * HD + HD] = val
            c_att(g * 2 + pair).start()

    step(0, [(0, k)], first=True)
    f_prev(0)
    f_one(0)

    @pl.when(tier_y)
    def _():
        @pl.when(yl == 1)
        def _():
            s_y.wait_recv()

        @pl.when(z == 0)
        def _():
            for c in s_z:
                c.start()

    step(1, [(0, k)], first=True)
    special = jnp.where(k == 0, 4, 0)

    def wait_special(g):
        @pl.when(k == 1)
        def _():
            wait_slot(g, 0)

        @pl.when(k == 0)
        def _():
            wait_slot(g, 9)

    wait_special(0)
    step(0, [(special, 0), (4, 1)])
    f_three(0)
    f_prev(1)

    @pl.when(tier_z)
    def _():
        @pl.when(z > 0)
        def _():
            s_z[0].wait_recv()

        s_k.start()

    wait_slot(0, 2 + (1 - k))
    step(0, [(1, 0), (1, 1)])
    f_one(1)
    f_two(0)
    for c in w3:
        c.wait_recv()
    for c in w4:
        c.start()
    wait_slot(0, 6 + (1 - k))
    step(0, [(3, 0), (3, 1)])
    f_three(1)
    wait_slot(0, 4 + (1 - k))
    step(0, [(2, 0), (2, 1)])

    @pl.when(k == 1)
    def _():
        s_k.wait_recv()

    finish(0)
    wait_special(1)
    step(1, [(special, 0), (4, 1)])
    f_two(1)
    for c in w4:
        c.wait_recv()
    w5.start()
    wait_slot(1, 2 + (1 - k))
    step(1, [(1, 0), (1, 1)])
    wait_slot(1, 6 + (1 - k))
    step(1, [(3, 0), (3, 1)])
    wait_slot(1, 4 + (1 - k))
    step(1, [(2, 0), (2, 1)])
    finish(1)

    own_copy.wait()
    w5.wait_recv()
    NT_ = 512

    def proj_own(n, c):
        cols = pl.ds(pl.multiple_of(n * NT_, NT_), NT_)
        y = None
        for pr in range(4):
            o = jnp.dot(att_v[pr], wown_v[pr * 256 : pr * 256 + 256, cols], preferred_element_type=F32)
            y = o if y is None else y + o
        o0_v[:, cols] = y.astype(BF16)
        return c

    lax.fori_loop(0, 4, proj_own, 0)

    def wrows(pr, cols):
        return wpeer_v[pl.ds(pr * 16, 16), :, cols].reshape(256, NT_)

    for pr in range(2):
        c_att(pr).wait_recv()

    def proj_first(n, c):
        cols = pl.ds(pl.multiple_of(n * NT_, NT_), NT_)
        y = jnp.dot(attp_v[0], wrows(0, cols), preferred_element_type=F32)
        o1_v[:, cols] = y + jnp.dot(attp_v[1], wrows(1, cols), preferred_element_type=F32)
        return c

    lax.fori_loop(0, 4, proj_first, 0)
    for pr in range(2, 4):
        c_att(pr).wait_recv()

    def ocopy(n):
        cols = pl.ds(pl.multiple_of(n * NT_, NT_), NT_)
        return pltpu.make_async_copy(out_v.at[:, cols], out_hbm.at[:, cols], out_sem.at[n])

    def proj_last(n, c):
        cols = pl.ds(pl.multiple_of(n * NT_, NT_), NT_)
        y = jnp.dot(attp_v[2], wrows(2, cols), preferred_element_type=F32)
        y = y + jnp.dot(attp_v[3], wrows(3, cols), preferred_element_type=F32)
        y = (y + o1_v[:, cols]).astype(BF16).astype(F32)
        base = x_v[:, pl.ds(pl.multiple_of(j * 2048 + n * NT_, NT_), NT_)].astype(F32)
        out_v[:, cols] = (base + (o0_v[:, cols].astype(F32) + y)).astype(BF16)
        ocopy(n).start()
        return c

    lax.fori_loop(0, 4, proj_last, 0)

    for g in range(2):
        wait_sends(g)
    w0.wait_send()
    w1.wait_send()
    for c in w2 + w3 + w4:
        c.wait_send()
    w5.wait_send()

    @pl.when(is_root)
    def _():
        for c in s_x:
            c.wait_send()

    @pl.when(tier_x)
    def _():
        s_y.wait_send()

    @pl.when(tier_y)
    def _():
        for c in s_z:
            c.wait_send()

    @pl.when(tier_z)
    def _():
        s_k.wait_send()

    for pr in range(4):
        c_att(pr).wait_send()
    for n in range(4):
        ocopy(n).wait()


def local(tokens, norm_gain, w_query, w_key, w_value, w_out, window, sink_count, sink_bias):
    any_ = pl.BlockSpec(memory_space=pl.ANY)
    smem = pl.BlockSpec(memory_space=pltpu.SMEM)
    vmem = pl.BlockSpec(memory_space=pltpu.VMEM)
    dma = pltpu.SemaphoreType.DMA
    return pl.pallas_call(
        kernel,
        out_shape=jax.ShapeDtypeStruct((T, 2048), BF16),
        in_specs=[any_, vmem, any_, any_, any_, any_, smem, smem, smem],
        out_specs=any_,
        scratch_shapes=[
            pltpu.VMEM((T, D), BF16),
            pltpu.VMEM((T, D), BF16),
            pltpu.VMEM((D, 1024), BF16),
            pltpu.VMEM((D, 512), BF16),
            pltpu.VMEM((1024, 2048), BF16),
            pltpu.VMEM((64, 16, 2048), BF16),
            pltpu.VMEM((10, 2, T, 256), BF16),
            pltpu.VMEM((2, SROWS, 256), BF16),
            pltpu.VMEM((8, T, 256), BF16),
            pltpu.VMEM((8, T, 256), F32),
            pltpu.VMEM((8, T, HD), F32),
            pltpu.VMEM((T, T), jnp.int32),
            pltpu.VMEM((4, T, 256), BF16),
            pltpu.VMEM((4, T, 256), BF16),
            pltpu.VMEM((T, 2048), BF16),
            pltpu.VMEM((T, 2048), F32),
            pltpu.VMEM((T, 2048), BF16),
            dma((13,)),
            dma((2, N_HALO_SEND)),
            dma((2, 10)),
            dma((10,)),
            dma((10,)),
            dma((8,)),
            dma((4,)),
            dma((4,)),
            dma((4,)),
            dma((4,)),
        ],
        compiler_params=pltpu.CompilerParams(
            has_side_effects=True, vmem_limit_bytes=64 * 1024 * 1024 - 65536
        ),
        name="block",
    )(tokens, norm_gain.reshape(1, D), w_query, w_key, w_value, w_out, window, sink_count, sink_bias)


def solution(mesh):
    in_specs = (
        P("seq", None),
        P(),
        P(None, "head"),
        P(None, "head"),
        P(None, "head"),
        P("head", None),
        P("head"),
        P("head"),
        P("head"),
    )
    return jax.shard_map(local, mesh=mesh, in_specs=in_specs, out_specs=P("seq", "head"), check_vma=False)
```

```python
import functools

import jax
import jax.numpy as jnp
from jax import lax
from jax.experimental import pallas as pl
from jax.experimental.pallas import tpu as pltpu
from jax.sharding import PartitionSpec as P

MESH = pl.DeviceIdType.MESH
HD = 128
T = 512
D = 4096
SINK = 4
SROWS = 16
EPS = 1e-05
scope = jax.named_scope
LOG2E = 1.4426950408889634
CSCALE = LOG2E * HD ** (-0.5)
NEG = -1e30
F32 = jnp.float32
BF16 = jnp.bfloat16
VR = 144

S_PREV, S_POS, S_NEG, S_FPOS, S_FNEG, S_D2D = 0, 1, 2, 3, 4, 5
N_HALO_SEND = S_D2D + 5


def kernel(
    x_hbm, gain_ref, wq_hbm, wk_hbm, wv_hbm, wo_hbm, win_ref, cnt_ref, bias_ref,
    out_hbm,
    x_v, n_v, wq_v, wkv_v, wown_v, wpeer_v, kv_v, sink_v, q_v, acc_v, m_v, rel_v, sa_v, sb_v,
    att_v, attp_v, o0_v, o1_v, out_v,
    in_sem, hsend, hrecv, wsend, wrecv, ssend, srecv, asend, arecv, out_sem,
):
    seq = lax.axis_index("seq")
    j = lax.axis_index("head")
    k = seq % 2
    x = (seq // 2) % 4
    r = seq // 8
    yl = r % 2
    z = r // 2
    peer = 1 - j

    def at(z_, yl_, x_, k_):
        return ((z_ * 2 + yl_) * 4 + x_) * 2 + k_

    sib = (at(z, yl, x, 1 - k), j)
    rn = (r + 1) % 8
    next_row = (rn * 8 + x * 2 + k, j)
    xp = (at(z, yl, (x + 1) % 4, k), j)
    xm = (at(z, yl, (x + 3) % 4, k), j)
    x2 = (at(z, yl, (x + 2) % 4, k), j)
    zp = (at((z + 1) % 4, yl, x, k), j)
    zm = (at((z + 3) % 4, yl, x, k), j)
    yo = (at(z, 1 - yl, x, k), j)
    head_peer = (seq, peer)

    def rcopy(src, dst, ss, rs, dev):
        return pltpu.make_async_remote_copy(
            src_ref=src, dst_ref=dst, send_sem=ss, recv_sem=rs, device_id=dev, device_id_type=MESH
        )

    def xcopy(i):
        rows = pl.ds(i * 128, 128)
        return pltpu.make_async_copy(x_hbm.at[rows], x_v.at[rows], in_sem.at[i])

    def kvcopy(i):
        g, w = i // 2, i % 2
        src = wk_hbm if w == 0 else wv_hbm
        return pltpu.make_async_copy(
            src.at[:, pl.ds(g * HD, HD)], wkv_v.at[:, pl.ds(i * HD, HD)], in_sem.at[4 + i]
        )

    def qcopy(i):
        cols = pl.ds(i * 256, 256)
        return pltpu.make_async_copy(wq_hbm.at[:, cols], wq_v.at[:, cols], in_sem.at[8 + i])

    own_copy = pltpu.make_async_copy(
        wo_hbm.at[:, pl.ds(pl.multiple_of(j * 2048, 2048), 2048)], wown_v, in_sem.at[12]
    )
    for i in range(4):
        xcopy(i).start()
    for i in range(4):
        kvcopy(i).start()
    for i in range(4):
        qcopy(i).start()
    own_copy.start()

    z2 = (at((z + 2) % 4, yl, x, k), j)
    prev_row = (((r + 7) % 8) * 8 + x * 2 + k, j)
    barrier = pltpu.get_barrier_semaphore()
    for dev in (sib, prev_row, xp, xm, x2, zp, zm, z2, yo, head_peer):
        pl.semaphore_signal(barrier, inc=1, device_id=dev, device_id_type=MESH)

    L = ((k * 4 + z) * 4 + x) * 2 + yl
    w0 = rcopy(
        wo_hbm.at[pl.ds(L * 16, 16), pl.ds(pl.multiple_of(peer * 2048, 2048), 2048)],
        wpeer_v.at[L], wsend.at[0], wrecv.at[0], head_peer,
    )

    w1 = rcopy(wpeer_v.at[L], wpeer_v.at[L], wsend.at[1], wrecv.at[1], yo)
    L2 = ((k * 4 + z) * 4 + x) * 2
    two = wpeer_v.at[pl.ds(L2, 2)]
    w2 = [rcopy(two, two, wsend.at[2 + i], wrecv.at[2 + i], d) for i, d in enumerate((xp, xm, x2))]
    L8 = (k * 4 + z) * 8
    eight = wpeer_v.at[pl.ds(L8, 8)]
    w3 = [rcopy(eight, eight, wsend.at[5 + i], wrecv.at[5 + i], d) for i, d in enumerate((zp, zm))]
    Lm = (k * 4 + (z + 3) % 4) * 8
    Lp = (k * 4 + (z + 1) % 4) * 8
    lo4 = wpeer_v.at[pl.ds(Lm, 4)]
    hi4 = wpeer_v.at[pl.ds(Lp + 4, 4)]
    w4 = [rcopy(lo4, lo4, wsend.at[7], wrecv.at[7], zp), rcopy(hi4, hi4, wsend.at[8], wrecv.at[8], zm)]
    half = wpeer_v.at[pl.ds(k * 32, 32)]
    w5 = rcopy(half, half, wsend.at[9], wrecv.at[9], sib)

    own_slot = k
    prev_slot = 8 + k

    def slot_copy(src_slot, dst_slot, g, srow, dev, rslot):
        return rcopy(kv_v.at[src_slot, g], kv_v.at[dst_slot, g], hsend.at[g, srow], hrecv.at[g, rslot], dev)

    def c_prev(g):
        return slot_copy(own_slot, 8 + k, g, S_PREV, next_row, 8 + k)

    def c_pos(g, src):
        return slot_copy(src, 2 + k, g, S_POS, xp, 2 + k)

    def c_neg(g, src):
        return slot_copy(src, 6 + k, g, S_NEG, xm, 6 + k)

    def c_fpos(g):
        return slot_copy(2 + k, 4 + k, g, S_FPOS, xp, 4 + k)

    def c_fneg(g):
        return slot_copy(6 + k, 4 + k, g, S_FNEG, xm, 4 + k)

    def c_d2d(g, d):
        return slot_copy(2 * d + k, 2 * d + k, g, S_D2D + d, sib, 2 * d + k)

    def wait_slot(g, s):
        slot_copy(s, s, g, S_PREV, sib, s).wait_recv()

    mid = (x == 1) | (x == 2)

    def start_own(g):
        c_prev(g).start()

        @pl.when(x < 3)
        def _():
            c_pos(g, own_slot).start()

        @pl.when(x == 0)
        def _():
            c_neg(g, own_slot).start()

        @pl.when(k == 0)
        def _():
            c_d2d(g, 0).start()

    def f_prev(g):
        wait_slot(g, 8 + k)

        @pl.when(x == 3)
        def _():
            c_pos(g, prev_slot).start()

        @pl.when(x > 0)
        def _():
            c_neg(g, prev_slot).start()

        @pl.when(k == 1)
        def _():
            c_d2d(g, 4).start()

    def f_one(g, early):
        @pl.when((x > 0) if early else (x == 0))
        def _():
            wait_slot(g, 2 + k)

            @pl.when(mid)
            def _():
                c_fpos(g).start()

            c_d2d(g, 1).start()

    def f_three(g):
        wait_slot(g, 6 + k)

        @pl.when(mid)
        def _():
            c_fneg(g).start()

        c_d2d(g, 3).start()

    def f_two(g):
        wait_slot(g, 4 + k)
        c_d2d(g, 2).start()

    def wait_sends(g):
        c_prev(g).wait_send()
        c_pos(g, own_slot).wait_send()
        c_neg(g, own_slot).wait_send()

        @pl.when(mid)
        def _():
            c_fpos(g).wait_send()
            c_fneg(g).wait_send()

        @pl.when(k == 0)
        def _():
            c_d2d(g, 0).wait_send()

        @pl.when(k == 1)
        def _():
            c_d2d(g, 4).wait_send()

        for d in (1, 2, 3):
            c_d2d(g, d).wait_send()

    sinks = sink_v.at[:]
    s_x = [rcopy(sinks, sinks, ssend.at[i], srecv.at[0], (at(0, 0, i + 1, 0), j)) for i in range(3)]
    s_y = rcopy(sinks, sinks, ssend.at[3], srecv.at[1], yo)
    s_z = [rcopy(sinks, sinks, ssend.at[4 + i], srecv.at[2], (at(i + 1, yl, x, 0), j)) for i in range(3)]
    s_k = rcopy(sinks, sinks, ssend.at[7], srecv.at[3], sib)
    is_root = seq == 0
    tier_x = (z == 0) & (yl == 0) & (k == 0)
    tier_y = (z == 0) & (k == 0)
    tier_z = k == 0

    def rel_rows(i, c):
        rows = pl.ds(i * 64, 64)
        a = lax.broadcasted_iota(jnp.int32, (64, T), 0) + i * 64
        b = lax.broadcasted_iota(jnp.int32, (64, T), 1)
        rel_v[rows, :] = b - a
        return c

    with scope("rel_rows"):
        lax.fori_loop(0, 8, rel_rows, 0)
    gain = gain_ref[...]
    with scope("barrier"):
        pl.semaphore_wait(barrier, 10)
    w0.start()

    def norm_rows(i, c):
        rows = pl.ds(i * 32, 32)
        xt = x_v[rows, :].astype(F32)
        ms = jnp.mean(xt * xt, axis=1, keepdims=True)
        n_v[rows, :] = (xt * lax.rsqrt(ms + EPS) * gain).astype(BF16)
        return c

    for i in range(4):
        with scope("xwait"):
            xcopy(i).wait()
        with scope("norm"):
            lax.fori_loop(i * 4, i * 4 + 4, norm_rows, 0)

    for g in range(2):
        with scope("kvwait"):
            kvcopy(2 * g).wait()
            kvcopy(2 * g + 1).wait()
        y = jnp.dot(n_v[...], wkv_v[:, g * 256 : g * 256 + 256], preferred_element_type=F32)
        kv_v[own_slot, g, :, 0:HD] = y[:, 0:HD].astype(BF16)
        for c in range(4):
            kv_v[own_slot, g, c * HD : c * HD + HD, HD : 2 * HD] = (
                y[c * HD : c * HD + HD, HD : 2 * HD].T.astype(BF16)
            )
        start_own(g)

        @pl.when(is_root)
        def _():
            sink_v[g] = y[:SROWS, :].astype(BF16)

    @pl.when(is_root)
    def _():
        for c in s_x:
            c.start()

    with scope("w0_wait_recv"):
        w0.wait_recv()
    w1.start()

    def q_tile(i):
        qcopy(2 * i).wait()
        qcopy(2 * i + 1).wait()
        y = jnp.dot(n_v[...], wq_v[:, i * 512 : i * 512 + 512], preferred_element_type=F32)
        for h in range(4):
            qt = y[:, h * HD : h * HD + HD].astype(BF16).astype(F32).T * CSCALE
            hi = qt.astype(BF16)
            q_v[4 * i + h, 0:HD, :] = hi
            q_v[4 * i + h, HD : 2 * HD, :] = (qt - hi.astype(F32)).astype(BF16)

    with scope("q0"):
        q_tile(0)

    @pl.when(tier_x)
    def _():
        @pl.when(jnp.logical_not(is_root))
        def _():
            s_x[0].wait_recv()

        s_y.start()

    ones = jnp.ones((VR - HD, T), BF16)

    def values_t(slot, g):
        vt = [kv_v[slot, g, c * HD : c * HD + HD, HD : 2 * HD] for c in range(4)]
        return jnp.concatenate([jnp.concatenate(vt, axis=1), ones], axis=0)

    def scores(g, h, slots, first, s_ref):
        q = q_v[h]
        w = win_ref[h]
        top = None
        for b, (d, kk) in enumerate(slots):
            dist = 2 * d + k - kk
            keys = kv_v[2 * d + kk, g, :, 0:HD]
            s = jnp.dot(jnp.concatenate([keys, keys], axis=1), q, preferred_element_type=F32)
            limit = jnp.where(seq >= dist, w - T * dist, -100000)
            rel = rel_v[...]
            seen = rel < limit
            if first:
                seen = seen & (rel >= 0)
            s = jnp.where(seen, s, NEG)
            s_ref[b * T : b * T + T, :] = s
            t = jnp.max(s, axis=0, keepdims=True)
            top = t if top is None else jnp.maximum(top, t)
        return top

    def weigh(g, h, slots, first, s_ref, top):
        if not first:
            old = m_v[h, 0:1, :]
            top = jnp.maximum(top, old)
        total = None
        for b, (d, kk) in enumerate(slots):
            p = jnp.exp2(s_ref[b * T : b * T + T, :] - top).astype(BF16)
            o = jnp.dot(values_t(2 * d + kk, g), p, preferred_element_type=F32)
            total = o if total is None else total + o
        if not first:
            total = total + acc_v[h] * jnp.exp2(old - top)
        acc_v[h] = total
        m_v[h] = jnp.broadcast_to(top, (8, T))

    def step(g, slots, first=False):
        base = g * 4

        def body(i, top):
            h = base + 2 * i
            top_b = scores(g, h + 1, slots, first, sb_v)
            weigh(g, h, slots, first, sa_v, top)
            top = scores(g, jnp.minimum(h + 2, base + 3), slots, first, sa_v)
            weigh(g, h + 1, slots, first, sb_v, top_b)
            return top

        lax.fori_loop(0, 2, body, scores(g, base, slots, first, sa_v))

    def c_att(pair):
        return rcopy(att_v.at[pair], attp_v.at[pair], asend.at[pair], arecv.at[pair], head_peer)

    def finish_head(g, h):
        ks = sink_v[g, :, 0:HD]
        vt = sink_v[g, :, HD : 2 * HD].astype(F32).T.astype(BF16)
        s = jnp.dot(jnp.concatenate([ks, ks], axis=1), q_v[h], preferred_element_type=F32)
        s = s + bias_ref[h] * LOG2E
        row = lax.broadcasted_iota(jnp.int32, (SROWS, T), 0)
        pos = lax.broadcasted_iota(jnp.int32, (SROWS, T), 1) + seq * T
        is_open = (row < cnt_ref[h]) & (row < SINK) & (row <= pos - win_ref[h])
        s = jnp.where(is_open, s, NEG)
        old = m_v[h, 0:1, :]
        top = jnp.maximum(jnp.max(s, axis=0, keepdims=True), old)
        p = jnp.exp2(s - top)
        scale = jnp.exp2(old - top)
        total = acc_v[h, HD : HD + 1, :] * scale + jnp.sum(p, axis=0, keepdims=True)
        o = acc_v[h, 0:HD, :] * scale + jnp.dot(vt, p.astype(BF16), preferred_element_type=F32)
        return (o / total).T.astype(BF16)

    def finish(g):
        for pair in range(2):
            for h in range(2):
                att_v[g * 2 + pair, :, h * HD : h * HD + HD] = finish_head(g, g * 4 + pair * 2 + h)
            c_att(g * 2 + pair).start()

    special = jnp.where(k == 0, 4, 0)

    def wait_special(g):
        @pl.when(k == 1)
        def _():
            wait_slot(g, 0)

        @pl.when(k == 0)
        def _():
            wait_slot(g, 9)

    with scope("q1"):
        q_tile(1)
    with scope("own0"):
        step(0, [(0, k)], first=True)
    with scope("f_prev0"):
        f_prev(0)
    with scope("f_one0"):
        f_one(0, True)
    with scope("w1_wait_recv"):
        w1.wait_recv()
    for c in w2:
        c.start()
    with scope("own1"):
        step(1, [(0, k)], first=True)

    @pl.when(tier_y)
    def _():
        @pl.when(yl == 1)
        def _():
            s_y.wait_recv()

        for c in s_z:
            c.start()

    with scope("f_prev1"):
        f_prev(1)
    with scope("f_one1"):
        f_one(1, True)
    with scope("wsp0"):
        wait_special(0)
    with scope("step0sp"):
        step(0, [(special, 0), (4, 1)])
    with scope("w2wait"):
        for c in w2:
            c.wait_recv()
    for c in w3:
        c.start()
    with scope("f_one0b"):
        f_one(0, False)
    with scope("f_three0"):
        f_three(0)
    with scope("w0_1"):
        wait_slot(0, 2 + (1 - k))
    with scope("step0_1"):
        step(0, [(1, 0), (1, 1)])

    @pl.when(tier_z)
    def _():
        @pl.when(z > 0)
        def _():
            s_z[0].wait_recv()

        s_k.start()

    with scope("f_one1b"):
        f_one(1, False)
    with scope("f_three1"):
        f_three(1)
    with scope("w0_3"):
        wait_slot(0, 6 + (1 - k))
    with scope("step0_3"):
        step(0, [(3, 0), (3, 1)])
    with scope("f_two0"):
        f_two(0)
    with scope("w3wait"):
        for c in w3:
            c.wait_recv()
    for c in w4:
        c.start()
    with scope("w0_2"):
        wait_slot(0, 4 + (1 - k))
    with scope("step0_2"):
        step(0, [(2, 0), (2, 1)])

    @pl.when(k == 1)
    def _():
        s_k.wait_recv()

    with scope("finish0"):
        finish(0)
    with scope("w1_1"):
        wait_special(1)
        wait_slot(1, 2 + (1 - k))
    with scope("step1a"):
        step(1, [(special, 0), (4, 1), (1, 0)])
    with scope("f_two1"):
        f_two(1)
    with scope("w4wait"):
        for c in w4:
            c.wait_recv()
    w5.start()
    with scope("w1_3"):
        wait_slot(1, 6 + (1 - k))
    with scope("step1b"):
        step(1, [(1, 1), (3, 0), (3, 1)])
    with scope("w1_2"):
        wait_slot(1, 4 + (1 - k))
    with scope("step1c"):
        step(1, [(2, 0), (2, 1)])
    with scope("finish1"):
        finish(1)

    with scope("own_copy_wait"):
        own_copy.wait()
    with scope("w5_wait_recv"):
        w5.wait_recv()
    NT_ = 512

    def proj_own(n, c):
        cols = pl.ds(pl.multiple_of(n * NT_, NT_), NT_)
        y = None
        for pr in range(4):
            o = jnp.dot(att_v[pr], wown_v[pr * 256 : pr * 256 + 256, cols], preferred_element_type=F32)
            y = o if y is None else y + o
        o0_v[:, cols] = y.astype(BF16)
        return c

    with scope("proj_own"):
        lax.fori_loop(0, 4, proj_own, 0)

    def wrows(pr, cols):
        return wpeer_v[pl.ds(pr * 16, 16), :, cols].reshape(256, NT_)

    with scope("att01wait"):
        for pr in range(2):
            c_att(pr).wait_recv()

    def proj_first(n, c):
        cols = pl.ds(pl.multiple_of(n * NT_, NT_), NT_)
        y = jnp.dot(attp_v[0], wrows(0, cols), preferred_element_type=F32)
        o1_v[:, cols] = y + jnp.dot(attp_v[1], wrows(1, cols), preferred_element_type=F32)
        return c

    with scope("proj_first"):
        lax.fori_loop(0, 4, proj_first, 0)
    with scope("att23wait"):
        for pr in range(2, 4):
            c_att(pr).wait_recv()

    def ocopy(n):
        cols = pl.ds(pl.multiple_of(n * NT_, NT_), NT_)
        return pltpu.make_async_copy(out_v.at[:, cols], out_hbm.at[:, cols], out_sem.at[n])

    def proj_last(n, c):
        cols = pl.ds(pl.multiple_of(n * NT_, NT_), NT_)
        y = jnp.dot(attp_v[2], wrows(2, cols), preferred_element_type=F32)
        y = y + jnp.dot(attp_v[3], wrows(3, cols), preferred_element_type=F32)
        y = (y + o1_v[:, cols]).astype(BF16).astype(F32)
        base = x_v[:, pl.ds(pl.multiple_of(j * 2048 + n * NT_, NT_), NT_)].astype(F32)
        out_v[:, cols] = (base + (o0_v[:, cols].astype(F32) + y)).astype(BF16)
        ocopy(n).start()
        return c

    with scope("proj_last"):
        lax.fori_loop(0, 4, proj_last, 0)

    for g in range(2):
        wait_sends(g)
    w0.wait_send()
    w1.wait_send()
    for c in w2 + w3 + w4:
        c.wait_send()
    w5.wait_send()

    @pl.when(is_root)
    def _():
        for c in s_x:
            c.wait_send()

    @pl.when(tier_x)
    def _():
        s_y.wait_send()

    @pl.when(tier_y)
    def _():
        for c in s_z:
            c.wait_send()

    @pl.when(tier_z)
    def _():
        s_k.wait_send()

    for pr in range(4):
        c_att(pr).wait_send()
    for n in range(4):
        ocopy(n).wait()


def local(tokens, norm_gain, w_query, w_key, w_value, w_out, window, sink_count, sink_bias):
    any_ = pl.BlockSpec(memory_space=pl.ANY)
    smem = pl.BlockSpec(memory_space=pltpu.SMEM)
    vmem = pl.BlockSpec(memory_space=pltpu.VMEM)
    dma = pltpu.SemaphoreType.DMA
    return pl.pallas_call(
        kernel,
        out_shape=jax.ShapeDtypeStruct((T, 2048), BF16),
        in_specs=[any_, vmem, any_, any_, any_, any_, smem, smem, smem],
        out_specs=any_,
        scratch_shapes=[
            pltpu.VMEM((T, D), BF16),
            pltpu.VMEM((T, D), BF16),
            pltpu.VMEM((D, 1024), BF16),
            pltpu.VMEM((D, 512), BF16),
            pltpu.VMEM((1024, 2048), BF16),
            pltpu.VMEM((64, 16, 2048), BF16),
            pltpu.VMEM((10, 2, T, 256), BF16),
            pltpu.VMEM((2, SROWS, 256), BF16),
            pltpu.VMEM((8, 256, T), BF16),
            pltpu.VMEM((8, VR, T), F32),
            pltpu.VMEM((8, 8, T), F32),
            pltpu.VMEM((T, T), jnp.int32),
            pltpu.VMEM((3 * T, T), F32),
            pltpu.VMEM((3 * T, T), F32),
            pltpu.VMEM((4, T, 256), BF16),
            pltpu.VMEM((4, T, 256), BF16),
            pltpu.VMEM((T, 2048), BF16),
            pltpu.VMEM((T, 2048), F32),
            pltpu.VMEM((T, 2048), BF16),
            dma((13,)),
            dma((2, N_HALO_SEND)),
            dma((2, 10)),
            dma((10,)),
            dma((10,)),
            dma((8,)),
            dma((4,)),
            dma((4,)),
            dma((4,)),
            dma((4,)),
        ],
        compiler_params=pltpu.CompilerParams(
            has_side_effects=True, collective_id=0, vmem_limit_bytes=64 * 1024 * 1024 - 65536
        ),
        name="block",
    )(tokens, norm_gain.reshape(1, D), w_query, w_key, w_value, w_out, window, sink_count, sink_bias)


def solution(mesh):
    in_specs = (
        P("seq", None),
        P(),
        P(None, "head"),
        P(None, "head"),
        P(None, "head"),
        P("head", None),
        P("head"),
        P("head"),
        P("head"),
    )
    return jax.shard_map(local, mesh=mesh, in_specs=in_specs, out_specs=P("seq", "head"), check_vma=False)
```

```python
import functools

import jax
import jax.numpy as jnp
from jax import lax
from jax.experimental import pallas as pl
from jax.experimental.pallas import tpu as pltpu
from jax.sharding import PartitionSpec as P

MESH = pl.DeviceIdType.MESH
HD = 128
T = 512
D = 4096
SINK = 4
SROWS = 16
EPS = 1e-05
scope = jax.named_scope
LOG2E = 1.4426950408889634
CSCALE = LOG2E * HD ** (-0.5)
NEG = -1e30
F32 = jnp.float32
BF16 = jnp.bfloat16
VR = 144

S_PREV, S_POS, S_NEG, S_FPOS, S_FNEG, S_D2D = 0, 1, 2, 3, 4, 5
N_HALO_SEND = S_D2D + 5


def kernel(
    x_hbm, gain_ref, wq_hbm, wk_hbm, wv_hbm, wo_hbm, win_ref, cnt_ref, bias_ref,
    out_hbm,
    x_v, n_v, wq_v, wkv_v, wown_v, wpeer_v, kv_v, sink_v, q_v, acc_v, m_v, rel_v, sa_v, sb_v,
    att_v, attp_v, o0_v, o1_v, out_v,
    in_sem, hsend, hrecv, wsend, wrecv, ssend, srecv, asend, arecv, out_sem,
):
    seq = lax.axis_index("seq")
    j = lax.axis_index("head")
    k = seq % 2
    x = (seq // 2) % 4
    r = seq // 8
    yl = r % 2
    z = r // 2
    peer = 1 - j

    def at(z_, yl_, x_, k_):
        return ((z_ * 2 + yl_) * 4 + x_) * 2 + k_

    sib = (at(z, yl, x, 1 - k), j)
    rn = (r + 1) % 8
    next_row = (rn * 8 + x * 2 + k, j)
    xp = (at(z, yl, (x + 1) % 4, k), j)
    xm = (at(z, yl, (x + 3) % 4, k), j)
    x2 = (at(z, yl, (x + 2) % 4, k), j)
    zp = (at((z + 1) % 4, yl, x, k), j)
    zm = (at((z + 3) % 4, yl, x, k), j)
    yo = (at(z, 1 - yl, x, k), j)
    head_peer = (seq, peer)
    diag = (at(z, 1 - yl, x, k), peer)

    def rcopy(src, dst, ss, rs, dev):
        return pltpu.make_async_remote_copy(
            src_ref=src, dst_ref=dst, send_sem=ss, recv_sem=rs, device_id=dev, device_id_type=MESH
        )

    def xcopy(i):
        rows = pl.ds(i * 128, 128)
        return pltpu.make_async_copy(x_hbm.at[rows], x_v.at[rows], in_sem.at[i])

    def kvcopy(i):
        g, w = i // 2, i % 2
        src = wk_hbm if w == 0 else wv_hbm
        return pltpu.make_async_copy(
            src.at[:, pl.ds(g * HD, HD)], wkv_v.at[:, pl.ds(i * HD, HD)], in_sem.at[4 + i]
        )

    def qcopy(i):
        cols = pl.ds(i * 256, 256)
        return pltpu.make_async_copy(wq_hbm.at[:, cols], wq_v.at[:, cols], in_sem.at[8 + i])

    own_copy = pltpu.make_async_copy(
        wo_hbm.at[:, pl.ds(pl.multiple_of(j * 2048, 2048), 2048)], wown_v, in_sem.at[12]
    )
    for i in range(4):
        xcopy(i).start()
    for i in range(4):
        kvcopy(i).start()
    for i in range(4):
        qcopy(i).start()
    own_copy.start()

    z2 = (at((z + 2) % 4, yl, x, k), j)
    prev_row = (((r + 7) % 8) * 8 + x * 2 + k, j)
    barrier = pltpu.get_barrier_semaphore()
    for dev in (sib, prev_row, xp, xm, x2, zp, zm, z2, yo, head_peer, diag):
        pl.semaphore_signal(barrier, inc=1, device_id=dev, device_id_type=MESH)

    L4 = ((k * 4 + z) * 2 + yl) * 4
    w_src = wo_hbm.at[
        pl.ds(pl.multiple_of(L4 * 16, 64), 64), pl.ds(pl.multiple_of(peer * 2048, 2048), 2048)
    ]
    w0 = [
        rcopy(w_src, wpeer_v.at[pl.ds(pl.multiple_of(L4 * 16, 64), 64)], wsend.at[i], wrecv.at[i], d)
        for i, d in enumerate((head_peer, diag))
    ]

    def w_rows(first, count):
        return wpeer_v.at[pl.ds(pl.multiple_of(first * 16, 64), count * 16)]

    L8 = (k * 4 + z) * 8
    eight = w_rows(L8, 8)
    own_lo, own_hi = w_rows(L8, 4), w_rows(L8 + 4, 4)
    w3a = [rcopy(own_lo, own_lo, wsend.at[2], wrecv.at[2], zp), rcopy(own_hi, own_hi, wsend.at[3], wrecv.at[3], zm)]
    w3b = [rcopy(own_hi, own_hi, wsend.at[10], wrecv.at[10], zp), rcopy(own_lo, own_lo, wsend.at[11], wrecv.at[11], zm)]
    Lm = (k * 4 + (z + 3) % 4) * 8
    Lp = (k * 4 + (z + 1) % 4) * 8
    lo4 = w_rows(Lm, 4)
    hi4 = w_rows(Lp + 4, 4)
    w4 = [rcopy(lo4, lo4, wsend.at[4], wrecv.at[4], zp), rcopy(hi4, hi4, wsend.at[5], wrecv.at[5], zm)]
    w5 = []
    for i in range(4):
        part = w_rows((k * 4 + (z + (0, 1, 3, 2)[i]) % 4) * 8, 8)
        w5.append(rcopy(part, part, wsend.at[6 + i], wrecv.at[6 + i], sib))

    own_slot = k
    prev_slot = 8 + k

    def slot_copy(src_slot, dst_slot, g, srow, dev, rslot):
        return rcopy(kv_v.at[src_slot, g], kv_v.at[dst_slot, g], hsend.at[g, srow], hrecv.at[g, rslot], dev)

    def c_prev(g):
        return slot_copy(own_slot, 8 + k, g, S_PREV, next_row, 8 + k)

    def c_pos(g, src):
        return slot_copy(src, 2 + k, g, S_POS, xp, 2 + k)

    def c_neg(g, src):
        return slot_copy(src, 6 + k, g, S_NEG, xm, 6 + k)

    def c_fpos(g):
        return slot_copy(2 + k, 4 + k, g, S_FPOS, xp, 4 + k)

    def c_fneg(g):
        return slot_copy(6 + k, 4 + k, g, S_FNEG, xm, 4 + k)

    def c_d2d(g, d):
        return slot_copy(2 * d + k, 2 * d + k, g, S_D2D + d, sib, 2 * d + k)

    def wait_slot(g, s):
        slot_copy(s, s, g, S_PREV, sib, s).wait_recv()

    def start_own(g):
        @pl.when(r < 7)
        def _():
            c_prev(g).start()

        @pl.when((x < 3) | (r == 0))
        def _():
            c_pos(g, own_slot).start()

        @pl.when((x == 0) | (r == 0))
        def _():
            c_neg(g, own_slot).start()

        @pl.when(k == 0)
        def _():
            c_d2d(g, 0).start()

    def f_prev(g):
        @pl.when(r > 0)
        def _():
            wait_slot(g, 8 + k)

            @pl.when(x == 3)
            def _():
                c_pos(g, prev_slot).start()

            @pl.when(x > 0)
            def _():
                c_neg(g, prev_slot).start()

            @pl.when(k == 1)
            def _():
                c_d2d(g, 4).start()

    def f_one(g, early):
        @pl.when((x > 0) if early else (x == 0))
        def _():
            wait_slot(g, 2 + k)

            @pl.when(x < 3)
            def _():
                c_fpos(g).start()

            c_d2d(g, 1).start()

    def f_three(g, which):
        @pl.when(which)
        def _():
            wait_slot(g, 6 + k)

            @pl.when(x == 1)
            def _():
                c_fneg(g).start()

            c_d2d(g, 3).start()

    def f_two(g):
        wait_slot(g, 4 + k)
        c_d2d(g, 2).start()

    def wait_sends(g):
        @pl.when(r < 7)
        def _():
            c_prev(g).wait_send()

        c_pos(g, own_slot).wait_send()
        c_neg(g, own_slot).wait_send()

        @pl.when(x < 3)
        def _():
            c_fpos(g).wait_send()

        @pl.when(x == 1)
        def _():
            c_fneg(g).wait_send()

        @pl.when(k == 0)
        def _():
            c_d2d(g, 0).wait_send()

        @pl.when((k == 1) & (r > 0))
        def _():
            c_d2d(g, 4).wait_send()

        for d in (1, 2, 3):
            c_d2d(g, d).wait_send()

    sinks = sink_v.at[:]
    s_x = [rcopy(sinks, sinks, ssend.at[i], srecv.at[0], (at(0, 0, i + 1, 0), j)) for i in range(3)]
    s_y = rcopy(sinks, sinks, ssend.at[3], srecv.at[1], yo)
    s_z = [rcopy(sinks, sinks, ssend.at[4 + i], srecv.at[2], (at(i + 1, yl, x, 0), j)) for i in range(3)]
    s_k = rcopy(sinks, sinks, ssend.at[7], srecv.at[3], sib)
    is_root = seq == 0
    tier_x = (z == 0) & (yl == 0) & (k == 0)
    tier_y = (z == 0) & (k == 0)
    tier_z = k == 0

    def rel_rows(i, c):
        rows = pl.ds(i * 64, 64)
        a = lax.broadcasted_iota(jnp.int32, (64, T), 0) + i * 64
        b = lax.broadcasted_iota(jnp.int32, (64, T), 1)
        rel_v[rows, :] = b - a
        return c

    with scope("rel_rows"):
        lax.fori_loop(0, 8, rel_rows, 0)
    gain = gain_ref[...]

    def norm_rows(i, c):
        rows = pl.ds(i * 32, 32)
        xt = x_v[rows, :].astype(F32)
        ms = jnp.mean(xt * xt, axis=1, keepdims=True)
        n_v[rows, :] = (xt * lax.rsqrt(ms + EPS) * gain).astype(BF16)
        return c

    for i in range(4):
        with scope("xwait"):
            xcopy(i).wait()
        with scope("norm"):
            lax.fori_loop(i * 4, i * 4 + 4, norm_rows, 0)

    with scope("barrier"):
        pl.semaphore_wait(barrier, 11)

    with scope("kvwait"):
        for i in range(4):
            kvcopy(i).wait()
    with scope("kv"):
        y = jnp.dot(n_v[...], wkv_v[...], preferred_element_type=F32)
        for g in range(2):
            yg = y[:, g * 256 : g * 256 + 256]
            kv_v[own_slot, g, :, 0:HD] = yg[:, 0:HD].astype(BF16)
            for c in range(4):
                kv_v[own_slot, g, c * HD : c * HD + HD, HD : 2 * HD] = (
                    yg[c * HD : c * HD + HD, HD : 2 * HD].T.astype(BF16)
                )
            if g == 1:

                @pl.when(is_root)
                def _():
                    for e in range(2):
                        sink_v[e] = y[:SROWS, e * 256 : e * 256 + 256].astype(BF16)
                    for c in s_x:
                        c.start()

            start_own(g)
    def q_tile(i):
        qcopy(2 * i).wait()
        qcopy(2 * i + 1).wait()
        y = jnp.dot(n_v[...], wq_v[:, i * 512 : i * 512 + 512], preferred_element_type=F32)
        for h in range(4):
            qt = y[:, h * HD : h * HD + HD].astype(BF16).astype(F32).T * CSCALE
            hi = qt.astype(BF16)
            q_v[4 * i + h, 0:HD, :] = hi
            q_v[4 * i + h, HD : 2 * HD, :] = (qt - hi.astype(F32)).astype(BF16)

    with scope("q0"):
        q_tile(0)

    ones = jnp.ones((VR - HD, T), BF16)

    def values_t(slot, g):
        vt = [kv_v[slot, g, c * HD : c * HD + HD, HD : 2 * HD] for c in range(4)]
        return jnp.concatenate([jnp.concatenate(vt, axis=1), ones], axis=0)

    def scores(g, h, slots, first, s_ref):
        q = q_v[h]
        w = win_ref[h]
        top = None
        for b, (dist, place) in enumerate(slots):
            keys = kv_v[place, g, :, 0:HD]
            s = jnp.dot(jnp.concatenate([keys, keys], axis=1), q, preferred_element_type=F32)
            limit = jnp.where(seq >= dist, w - T * dist, -100000)
            rel = rel_v[...]
            seen = rel < limit
            if first:
                seen = seen & (rel >= 0)
            s = jnp.where(seen, s, NEG)
            s_ref[b * T : b * T + T, :] = s
            t = jnp.max(s, axis=0, keepdims=True)
            top = t if top is None else jnp.maximum(top, t)
        return top

    def weigh(g, h, slots, first, s_ref, top):
        if not first:
            old = m_v[h, 0:1, :]
            top = jnp.maximum(top, old)
        total = None
        for b, (_, place) in enumerate(slots):
            p = jnp.exp2(s_ref[b * T : b * T + T, :] - top).astype(BF16)
            o = jnp.dot(values_t(place, g), p, preferred_element_type=F32)
            total = o if total is None else total + o
        if not first:
            total = total + acc_v[h] * jnp.exp2(old - top)
        acc_v[h] = total
        m_v[h] = jnp.broadcast_to(top, (8, T))

    def step(g, slots, first=False):
        base = g * 4

        def body(i, top):
            h = base + 2 * i
            top_b = scores(g, h + 1, slots, first, sb_v)
            weigh(g, h, slots, first, sa_v, top)
            top = scores(g, jnp.minimum(h + 2, base + 3), slots, first, sa_v)
            weigh(g, h + 1, slots, first, sb_v, top_b)
            return top

        lax.fori_loop(0, 2, body, scores(g, base, slots, first, sa_v))

    def c_att(h):
        return rcopy(att_v.at[h], attp_v.at[h], asend.at[h], arecv.at[h], head_peer)

    def finish_head(g, h):
        ks = sink_v[g, :, 0:HD]
        vt = sink_v[g, :, HD : 2 * HD].astype(F32).T.astype(BF16)
        s = jnp.dot(jnp.concatenate([ks, ks], axis=1), q_v[h], preferred_element_type=F32)
        s = s + bias_ref[h] * LOG2E
        row = lax.broadcasted_iota(jnp.int32, (SROWS, T), 0)
        pos = lax.broadcasted_iota(jnp.int32, (SROWS, T), 1) + seq * T
        is_open = (row < cnt_ref[h]) & (row < SINK) & (row <= pos - win_ref[h])
        s = jnp.where(is_open, s, NEG)
        old = m_v[h, 0:1, :]
        top = jnp.maximum(jnp.max(s, axis=0, keepdims=True), old)
        p = jnp.exp2(s - top)
        scale = jnp.exp2(old - top)
        total = acc_v[h, HD : HD + 1, :] * scale + jnp.sum(p, axis=0, keepdims=True)
        o = acc_v[h, 0:HD, :] * scale + jnp.dot(vt, p.astype(BF16), preferred_element_type=F32)
        return (o / total).T.astype(BF16)

    def finish(g, heads=(0, 1, 2, 3)):
        for i in heads:
            att_v[g * 4 + i] = finish_head(g, g * 4 + i)
            c_att(g * 4 + i).start()

    def pair_steps(g, h0, steps):
        items = [(slots, h0 + i) for slots in steps for i in range(2)]
        bufs = (sa_v, sb_v)
        last = None
        for n, (slots, h) in enumerate(items):
            top = scores(g, h, slots, False, bufs[n % 2])
            if last is not None:
                weigh(*last)
            last = (g, h, slots, False, bufs[n % 2], top)
        weigh(*last)

    own = (0, own_slot)
    special = (jnp.where(k == 0, 8, 1), jnp.where((k == 0) & (r > 0), 8, 0))
    prev_odd = (7 + k, jnp.where(r == 0, k, 9))

    def slot(d, kk):
        return (2 * d + k - kk, 2 * d + kk)


    def wait_special(g):
        @pl.when(k == 1)
        def _():
            wait_slot(g, 0)

        @pl.when((k == 0) & (r > 0))
        def _():
            wait_slot(g, 9)

    with scope("q1"):
        q_tile(1)
    with scope("own0"):
        step(0, [own], first=True)
    with scope("f_prev0"):
        f_prev(0)
    with scope("f_one0"):
        f_one(0, True)
    for c in w0:
        c.start()
    with scope("own1"):
        step(1, [own], first=True)
    with scope("tier_x"):

        @pl.when(tier_x)
        def _():
            @pl.when(jnp.logical_not(is_root))
            def _():
                s_x[0].wait_recv()

            s_y.start()

    with scope("wsp0"):
        wait_special(0)
    with scope("step0sp"):
        step(0, [special, prev_odd])
    with scope("f_prev1"):
        f_prev(1)
    with scope("f_one0b"):
        f_one(0, False)
    with scope("f_three0"):
        f_three(0, x >= 0)
    with scope("f_one1"):
        f_one(1, True)
    with scope("w0_1"):
        wait_slot(0, 2 + (1 - k))
    with scope("step0_1"):
        step(0, [slot(1, 0), slot(1, 1)])
    with scope("tier_y"):

        @pl.when(tier_y)
        def _():
            @pl.when(yl == 1)
            def _():
                s_y.wait_recv()

            for c in s_z:
                c.start()

    with scope("f_three1a"):
        f_three(1, x == 1)
    with scope("w0_3"):
        wait_slot(0, 6 + (1 - k))
    with scope("step0_3"):
        step(0, [slot(3, 0), slot(3, 1)])
    with scope("w0wait"):
        for c in w0:
            c.wait_recv()
    for c in w3a + w3b:
        c.start()
    w5[0].start()
    with scope("tier_z"):

        @pl.when(tier_z)
        def _():
            @pl.when(z > 0)
            def _():
                s_z[0].wait_recv()

            s_k.start()

    with scope("wsp1"):
        wait_special(1)
    with scope("step1sp"):
        step(1, [special, prev_odd])
    with scope("f_two0"):
        f_two(0)
    with scope("f_one1b"):
        f_one(1, False)
    with scope("w0_2"):
        wait_slot(0, 4 + (1 - k))
    with scope("step0_2"):
        step(0, [slot(2, 0), slot(2, 1)])
    with scope("tier_k"):

        @pl.when(k == 1)
        def _():
            s_k.wait_recv()

    with scope("finish0"):
        finish(0)
    with scope("f_three1b"):
        f_three(1, x != 1)
    with scope("w3await"):
        for c in w3a:
            c.wait_recv()
    for c in w4:
        c.start()
    with scope("w1_1"):
        wait_slot(1, 2 + (1 - k))
        wait_slot(1, 6 + (1 - k))
    with scope("step1b"):
        step(1, [slot(1, 0), slot(1, 1), slot(3, 0)])
    with scope("f_two1"):
        f_two(1)
    with scope("w1_2"):
        wait_slot(1, 4 + (1 - k))
    tail = [[slot(3, 1), slot(2, 0), slot(2, 1)]]
    with scope("pairA"):
        pair_steps(1, 4, tail)
    with scope("finishA"):
        finish(1, (0, 1))
    with scope("pairB"):
        pair_steps(1, 6, tail)
    with scope("finishB"):
        finish(1, (2, 3))
    with scope("w3bwait"):
        for c in w3b:
            c.wait_recv()
    w5[1].start()
    w5[2].start()
    with scope("w4wait"):
        for c in w4:
            c.wait_recv()
    w5[3].start()
    with scope("own_copy_wait"):
        own_copy.wait()
    NT_ = 512

    def two_heads(ref, pr):
        return jnp.concatenate([ref[2 * pr], ref[2 * pr + 1]], axis=1)

    def proj_own(n, c):
        cols = pl.ds(pl.multiple_of(n * NT_, NT_), NT_)
        y = None
        for pr in range(4):
            o = jnp.dot(two_heads(att_v, pr), wown_v[pr * 256 : pr * 256 + 256, cols], preferred_element_type=F32)
            y = o if y is None else y + o
        o0_v[:, cols] = y.astype(BF16)
        return c

    with scope("proj_own"):
        lax.fori_loop(0, 4, proj_own, 0)

    def wrows(pr, cols):
        return wpeer_v[pr * 256 : pr * 256 + 256, cols]

    with scope("w5wait"):
        for i in range(4):
            part = w_rows(((1 - k) * 4 + (z + (0, 1, 3, 2)[i]) % 4) * 8, 8)
            rcopy(part, part, wsend.at[6 + i], wrecv.at[6 + i], sib).wait_recv()
    with scope("att01wait"):
        for h in range(4):
            c_att(h).wait_recv()

    def proj_first(n, c):
        cols = pl.ds(pl.multiple_of(n * NT_, NT_), NT_)
        y = jnp.dot(two_heads(attp_v, 0), wrows(0, cols), preferred_element_type=F32)
        o1_v[:, cols] = y + jnp.dot(two_heads(attp_v, 1), wrows(1, cols), preferred_element_type=F32)
        return c

    with scope("proj_first"):
        lax.fori_loop(0, 4, proj_first, 0)
    with scope("att23wait"):
        for h in range(4, 8):
            c_att(h).wait_recv()

    def ocopy(n):
        cols = pl.ds(pl.multiple_of(n * NT_, NT_), NT_)
        return pltpu.make_async_copy(out_v.at[:, cols], out_hbm.at[:, cols], out_sem.at[n])

    def proj_last(n, c):
        cols = pl.ds(pl.multiple_of(n * NT_, NT_), NT_)
        y = jnp.dot(two_heads(attp_v, 2), wrows(2, cols), preferred_element_type=F32)
        y = y + jnp.dot(two_heads(attp_v, 3), wrows(3, cols), preferred_element_type=F32)
        y = (y + o1_v[:, cols]).astype(BF16).astype(F32)
        base = x_v[:, pl.ds(pl.multiple_of(j * 2048 + n * NT_, NT_), NT_)].astype(F32)
        out_v[:, cols] = (base + (o0_v[:, cols].astype(F32) + y)).astype(BF16)
        ocopy(n).start()
        return c

    with scope("proj_last"):
        lax.fori_loop(0, 4, proj_last, 0)

    for g in range(2):
        wait_sends(g)
    for c in w0 + w3a + w3b + w4 + w5:
        c.wait_send()

    @pl.when(is_root)
    def _():
        for c in s_x:
            c.wait_send()

    @pl.when(tier_x)
    def _():
        s_y.wait_send()

    @pl.when(tier_y)
    def _():
        for c in s_z:
            c.wait_send()

    @pl.when(tier_z)
    def _():
        s_k.wait_send()

    for h in range(8):
        c_att(h).wait_send()
    for n in range(4):
        ocopy(n).wait()


def local(tokens, norm_gain, w_query, w_key, w_value, w_out, window, sink_count, sink_bias):
    any_ = pl.BlockSpec(memory_space=pl.ANY)
    smem = pl.BlockSpec(memory_space=pltpu.SMEM)
    vmem = pl.BlockSpec(memory_space=pltpu.VMEM)
    dma = pltpu.SemaphoreType.DMA
    return pl.pallas_call(
        kernel,
        out_shape=jax.ShapeDtypeStruct((T, 2048), BF16),
        in_specs=[any_, vmem, any_, any_, any_, any_, smem, smem, smem],
        out_specs=any_,
        scratch_shapes=[
            pltpu.VMEM((T, D), BF16),
            pltpu.VMEM((T, D), BF16),
            pltpu.VMEM((D, 1024), BF16),
            pltpu.VMEM((D, 512), BF16),
            pltpu.VMEM((1024, 2048), BF16),
            pltpu.VMEM((1024, 2048), BF16),
            pltpu.VMEM((10, 2, T, 256), BF16),
            pltpu.VMEM((2, SROWS, 256), BF16),
            pltpu.VMEM((8, 256, T), BF16),
            pltpu.VMEM((8, VR, T), F32),
            pltpu.VMEM((8, 8, T), F32),
            pltpu.VMEM((T, T), jnp.int32),
            pltpu.VMEM((3 * T, T), F32),
            pltpu.VMEM((3 * T, T), F32),
            pltpu.VMEM((8, T, HD), BF16),
            pltpu.VMEM((8, T, HD), BF16),
            pltpu.VMEM((T, 2048), BF16),
            pltpu.VMEM((T, 2048), F32),
            pltpu.VMEM((T, 2048), BF16),
            dma((13,)),
            dma((2, N_HALO_SEND)),
            dma((2, 10)),
            dma((12,)),
            dma((12,)),
            dma((8,)),
            dma((4,)),
            dma((8,)),
            dma((8,)),
            dma((4,)),
        ],
        compiler_params=pltpu.CompilerParams(
            has_side_effects=True, collective_id=0, vmem_limit_bytes=64 * 1024 * 1024 - 65536
        ),
        name="block",
    )(tokens, norm_gain.reshape(1, D), w_query, w_key, w_value, w_out, window, sink_count, sink_bias)


def solution(mesh):
    in_specs = (
        P("seq", None),
        P(),
        P(None, "head"),
        P(None, "head"),
        P(None, "head"),
        P("head", None),
        P("head"),
        P("head"),
        P("head"),
    )
    return jax.shard_map(local, mesh=mesh, in_specs=in_specs, out_specs=P("seq", "head"), check_vma=False)
```

```python
import functools

import jax
import jax.numpy as jnp
from jax import lax
from jax.experimental import pallas as pl
from jax.experimental.pallas import tpu as pltpu
from jax.sharding import PartitionSpec as P

MESH = pl.DeviceIdType.MESH
HD = 128
T = 512
D = 4096
SINK = 4
SROWS = 16
EPS = 1e-05
scope = jax.named_scope
LOG2E = 1.4426950408889634
CSCALE = LOG2E * HD ** (-0.5)
NEG = -1e30
F32 = jnp.float32
BF16 = jnp.bfloat16
VR = 144

S_PREV, S_POS, S_NEG, S_FPOS, S_FNEG, S_D2D = 0, 1, 2, 3, 4, 5
N_HALO_SEND = S_D2D + 5


def kernel(
    x_hbm, gain_ref, wq_hbm, wk_hbm, wv_hbm, wo_hbm, win_ref, cnt_ref, bias_ref,
    out_hbm,
    x_v, n_v, wq_v, wkv_v, wown_v, wpeer_v, kv_v, sink_v, q_v, acc_v, m_v, rel_v, sa_v, sb_v,
    att_v, attp_v, o0_v, o1_v, out_v,
    in_sem, hsend, hrecv, wsend, wrecv, ssend, srecv, asend, arecv, out_sem,
):
    seq = lax.axis_index("seq")
    j = lax.axis_index("head")
    k = seq % 2
    x = (seq // 2) % 4
    r = seq // 8
    yl = r % 2
    z = r // 2
    peer = 1 - j

    def at(z_, yl_, x_, k_):
        return ((z_ * 2 + yl_) * 4 + x_) * 2 + k_

    sib = (at(z, yl, x, 1 - k), j)
    rn = (r + 1) % 8
    next_row = (rn * 8 + x * 2 + k, j)
    xp = (at(z, yl, (x + 1) % 4, k), j)
    xm = (at(z, yl, (x + 3) % 4, k), j)
    x2 = (at(z, yl, (x + 2) % 4, k), j)
    zp = (at((z + 1) % 4, yl, x, k), j)
    zm = (at((z + 3) % 4, yl, x, k), j)
    yo = (at(z, 1 - yl, x, k), j)
    head_peer = (seq, peer)
    diag = (at(z, 1 - yl, x, k), peer)

    def rcopy(src, dst, ss, rs, dev):
        return pltpu.make_async_remote_copy(
            src_ref=src, dst_ref=dst, send_sem=ss, recv_sem=rs, device_id=dev, device_id_type=MESH
        )

    def xcopy(i):
        rows = pl.ds(i * 128, 128)
        return pltpu.make_async_copy(x_hbm.at[rows], x_v.at[rows], in_sem.at[i])

    def kvcopy(i):
        g, w = i // 2, i % 2
        src = wk_hbm if w == 0 else wv_hbm
        return pltpu.make_async_copy(
            src.at[:, pl.ds(g * HD, HD)], wkv_v.at[:, pl.ds(i * HD, HD)], in_sem.at[4 + i]
        )

    def qcopy(i):
        cols = pl.ds(i * 256, 256)
        return pltpu.make_async_copy(wq_hbm.at[:, cols], wq_v.at[:, cols], in_sem.at[8 + i])

    own_copy = pltpu.make_async_copy(
        wo_hbm.at[:, pl.ds(pl.multiple_of(j * 2048, 2048), 2048)], wown_v, in_sem.at[12]
    )
    for i in range(4):
        xcopy(i).start()
    for i in range(4):
        kvcopy(i).start()
    for i in range(4):
        qcopy(i).start()
    own_copy.start()

    z2 = (at((z + 2) % 4, yl, x, k), j)
    prev_row = (((r + 7) % 8) * 8 + x * 2 + k, j)
    barrier = pltpu.get_barrier_semaphore()
    for dev in (sib, prev_row, xp, xm, x2, zp, zm, z2, yo, head_peer, diag):
        pl.semaphore_signal(barrier, inc=1, device_id=dev, device_id_type=MESH)

    L4 = ((k * 4 + z) * 2 + yl) * 4
    w_src = wo_hbm.at[
        pl.ds(pl.multiple_of(L4 * 16, 64), 64), pl.ds(pl.multiple_of(peer * 2048, 2048), 2048)
    ]
    w0 = [
        rcopy(w_src, wpeer_v.at[pl.ds(pl.multiple_of(L4 * 16, 64), 64)], wsend.at[i], wrecv.at[i], d)
        for i, d in enumerate((head_peer, diag))
    ]

    def w_rows(first, count):
        return wpeer_v.at[pl.ds(pl.multiple_of(first * 16, 64), count * 16)]

    L8 = (k * 4 + z) * 8
    eight = w_rows(L8, 8)
    own_lo, own_hi = w_rows(L8, 4), w_rows(L8 + 4, 4)
    w3a = [rcopy(own_lo, own_lo, wsend.at[2], wrecv.at[2], zp), rcopy(own_hi, own_hi, wsend.at[3], wrecv.at[3], zm)]
    w3b = [rcopy(own_hi, own_hi, wsend.at[10], wrecv.at[10], zp), rcopy(own_lo, own_lo, wsend.at[11], wrecv.at[11], zm)]
    Lm = (k * 4 + (z + 3) % 4) * 8
    Lp = (k * 4 + (z + 1) % 4) * 8
    lo4 = w_rows(Lm, 4)
    hi4 = w_rows(Lp + 4, 4)
    w4 = [rcopy(lo4, lo4, wsend.at[4], wrecv.at[4], zp), rcopy(hi4, hi4, wsend.at[5], wrecv.at[5], zm)]
    w5 = []
    for i in range(4):
        part = w_rows((k * 4 + (z + (0, 1, 3, 2)[i]) % 4) * 8, 8)
        w5.append(rcopy(part, part, wsend.at[6 + i], wrecv.at[6 + i], sib))

    own_slot = k
    prev_slot = 8 + k

    def slot_copy(src_slot, dst_slot, g, srow, dev, rslot):
        return rcopy(kv_v.at[src_slot, g], kv_v.at[dst_slot, g], hsend.at[g, srow], hrecv.at[g, rslot], dev)

    def c_prev(g):
        return slot_copy(own_slot, 8 + k, g, S_PREV, next_row, 8 + k)

    def c_pos(g, src):
        return slot_copy(src, 2 + k, g, S_POS, xp, 2 + k)

    def c_neg(g, src):
        return slot_copy(src, 6 + k, g, S_NEG, xm, 6 + k)

    def c_fpos(g):
        return slot_copy(2 + k, 4 + k, g, S_FPOS, xp, 4 + k)

    def c_fneg(g):
        return slot_copy(6 + k, 4 + k, g, S_FNEG, xm, 4 + k)

    def c_d2d(g, d):
        return slot_copy(2 * d + k, 2 * d + k, g, S_D2D + d, sib, 2 * d + k)

    def wait_slot(g, s):
        slot_copy(s, s, g, S_PREV, sib, s).wait_recv()

    def start_own(g):
        @pl.when(r < 7)
        def _():
            c_prev(g).start()

        @pl.when((x < 3) | (r == 0))
        def _():
            c_pos(g, own_slot).start()

        @pl.when((x == 0) | (r == 0))
        def _():
            c_neg(g, own_slot).start()

        @pl.when(k == 0)
        def _():
            c_d2d(g, 0).start()

    def f_prev(g, which):
        @pl.when((r > 0) & which)
        def _():
            wait_slot(g, 8 + k)

            @pl.when(x == 3)
            def _():
                c_pos(g, prev_slot).start()

            @pl.when(x > 0)
            def _():
                c_neg(g, prev_slot).start()

            @pl.when(k == 1)
            def _():
                c_d2d(g, 4).start()

    def f_one(g, early):
        @pl.when((x > 0) if early else (x == 0))
        def _():
            wait_slot(g, 2 + k)

            @pl.when(x < 3)
            def _():
                c_fpos(g).start()

            c_d2d(g, 1).start()

    def f_three(g, which):
        @pl.when(which)
        def _():
            wait_slot(g, 6 + k)

            @pl.when(x == 1)
            def _():
                c_fneg(g).start()

            c_d2d(g, 3).start()

    def f_two(g):
        wait_slot(g, 4 + k)
        c_d2d(g, 2).start()

    def wait_sends(g):
        @pl.when(r < 7)
        def _():
            c_prev(g).wait_send()

        c_pos(g, own_slot).wait_send()
        c_neg(g, own_slot).wait_send()

        @pl.when(x < 3)
        def _():
            c_fpos(g).wait_send()

        @pl.when(x == 1)
        def _():
            c_fneg(g).wait_send()

        @pl.when(k == 0)
        def _():
            c_d2d(g, 0).wait_send()

        @pl.when((k == 1) & (r > 0))
        def _():
            c_d2d(g, 4).wait_send()

        for d in (1, 2, 3):
            c_d2d(g, d).wait_send()

    sinks = sink_v.at[:]
    s_x = [rcopy(sinks, sinks, ssend.at[i], srecv.at[0], (at(0, 0, i + 1, 0), j)) for i in range(3)]
    s_y = rcopy(sinks, sinks, ssend.at[3], srecv.at[1], yo)
    s_z = [rcopy(sinks, sinks, ssend.at[4 + i], srecv.at[2], (at(i + 1, yl, x, 0), j)) for i in range(3)]
    s_k = rcopy(sinks, sinks, ssend.at[7], srecv.at[3], sib)
    is_root = seq == 0
    tier_x = (z == 0) & (yl == 0) & (k == 0)
    tier_y = (z == 0) & (k == 0)
    tier_z = k == 0

    def rel_rows(i, c):
        rows = pl.ds(i * 64, 64)
        a = lax.broadcasted_iota(jnp.int32, (64, T), 0) + i * 64
        b = lax.broadcasted_iota(jnp.int32, (64, T), 1)
        rel_v[rows, :] = b - a
        return c

    with scope("rel_rows"):
        lax.fori_loop(0, 8, rel_rows, 0)
    gain = gain_ref[...]

    def norm_rows(i, c):
        rows = pl.ds(i * 32, 32)
        xt = x_v[rows, :].astype(F32)
        ms = jnp.mean(xt * xt, axis=1, keepdims=True)
        n_v[rows, :] = (xt * lax.rsqrt(ms + EPS) * gain).astype(BF16)
        return c

    for i in range(4):
        with scope("xwait"):
            xcopy(i).wait()
        with scope("norm"):
            lax.fori_loop(i * 4, i * 4 + 4, norm_rows, 0)

    with scope("barrier"):
        pl.semaphore_wait(barrier, 11)

    with scope("kvwait"):
        for i in range(4):
            kvcopy(i).wait()
    with scope("kv"):
        y = jnp.dot(n_v[...], wkv_v[...], preferred_element_type=F32)
        for g in range(2):
            yg = y[:, g * 256 : g * 256 + 256]
            kv_v[own_slot, g, :, 0:HD] = yg[:, 0:HD].astype(BF16)
            for c in range(4):
                kv_v[own_slot, g, c * HD : c * HD + HD, HD : 2 * HD] = (
                    yg[c * HD : c * HD + HD, HD : 2 * HD].T.astype(BF16)
                )
            if g == 1:

                @pl.when(is_root)
                def _():
                    for e in range(2):
                        sink_v[e] = y[:SROWS, e * 256 : e * 256 + 256].astype(BF16)
                    for c in s_x:
                        c.start()

            start_own(g)
    def q_tile(i):
        qcopy(2 * i).wait()
        qcopy(2 * i + 1).wait()
        y = jnp.dot(n_v[...], wq_v[:, i * 512 : i * 512 + 512], preferred_element_type=F32)
        for h in range(4):
            qt = y[:, h * HD : h * HD + HD].astype(BF16).astype(F32).T * CSCALE
            hi = qt.astype(BF16)
            q_v[4 * i + h, 0:HD, :] = hi
            q_v[4 * i + h, HD : 2 * HD, :] = (qt - hi.astype(F32)).astype(BF16)

    with scope("q0"):
        q_tile(0)

    ones = jnp.ones((VR - HD, T), BF16)

    def values_t(slot, g):
        vt = [kv_v[slot, g, c * HD : c * HD + HD, HD : 2 * HD] for c in range(4)]
        return jnp.concatenate([jnp.concatenate(vt, axis=1), ones], axis=0)

    def scores(g, h, slots, first, s_ref):
        q = q_v[h]
        w = win_ref[h]
        top = None
        for b, (dist, place) in enumerate(slots):
            keys = kv_v[place, g, :, 0:HD]
            s = jnp.dot(jnp.concatenate([keys, keys], axis=1), q, preferred_element_type=F32)
            limit = jnp.where(seq >= dist, w - T * dist, -100000)
            rel = rel_v[...]
            seen = rel < limit
            if first:
                seen = seen & (rel >= 0)
            s = jnp.where(seen, s, NEG)
            s_ref[b * T : b * T + T, :] = s
            t = jnp.max(s, axis=0, keepdims=True)
            top = t if top is None else jnp.maximum(top, t)
        return top

    def weigh(g, h, slots, first, s_ref, top):
        if not first:
            old = m_v[h, 0:1, :]
            top = jnp.maximum(top, old)
        total = None
        for b, (_, place) in enumerate(slots):
            p = jnp.exp2(s_ref[b * T : b * T + T, :] - top).astype(BF16)
            o = jnp.dot(values_t(place, g), p, preferred_element_type=F32)
            total = o if total is None else total + o
        if not first:
            total = total + acc_v[h] * jnp.exp2(old - top)
        acc_v[h] = total
        m_v[h] = jnp.broadcast_to(top, (8, T))

    def step(g, slots, first=False):
        base = g * 4

        def body(i, top):
            h = base + 2 * i
            top_b = scores(g, h + 1, slots, first, sb_v)
            weigh(g, h, slots, first, sa_v, top)
            top = scores(g, jnp.minimum(h + 2, base + 3), slots, first, sa_v)
            weigh(g, h + 1, slots, first, sb_v, top_b)
            return top

        lax.fori_loop(0, 2, body, scores(g, base, slots, first, sa_v))

    def c_att(h):
        return rcopy(att_v.at[h], attp_v.at[h], asend.at[h], arecv.at[h], head_peer)

    def finish_head(g, h):
        ks = sink_v[g, :, 0:HD]
        vt = sink_v[g, :, HD : 2 * HD].astype(F32).T.astype(BF16)
        s = jnp.dot(jnp.concatenate([ks, ks], axis=1), q_v[h], preferred_element_type=F32)
        s = s + bias_ref[h] * LOG2E
        row = lax.broadcasted_iota(jnp.int32, (SROWS, T), 0)
        pos = lax.broadcasted_iota(jnp.int32, (SROWS, T), 1) + seq * T
        is_open = (row < cnt_ref[h]) & (row < SINK) & (row <= pos - win_ref[h])
        s = jnp.where(is_open, s, NEG)
        old = m_v[h, 0:1, :]
        top = jnp.maximum(jnp.max(s, axis=0, keepdims=True), old)
        p = jnp.exp2(s - top)
        scale = jnp.exp2(old - top)
        total = acc_v[h, HD : HD + 1, :] * scale + jnp.sum(p, axis=0, keepdims=True)
        o = acc_v[h, 0:HD, :] * scale + jnp.dot(vt, p.astype(BF16), preferred_element_type=F32)
        return (o / total).T.astype(BF16)

    def finish(g, heads=(0, 1, 2, 3)):
        for i in heads:
            att_v[g * 4 + i] = finish_head(g, g * 4 + i)
            c_att(g * 4 + i).start()

    def pair_steps(g, h0, steps):
        items = [(slots, h0 + i) for slots in steps for i in range(2)]
        bufs = (sa_v, sb_v)
        last = None
        for n, (slots, h) in enumerate(items):
            top = scores(g, h, slots, False, bufs[n % 2])
            if last is not None:
                weigh(*last)
            last = (g, h, slots, False, bufs[n % 2], top)
        weigh(*last)

    own = (0, own_slot)
    special = (jnp.where(k == 0, 8, 1), jnp.where((k == 0) & (r > 0), 8, 0))
    prev_odd = (7 + k, jnp.where(r == 0, k, 9))

    def slot(d, kk):
        return (2 * d + k - kk, 2 * d + kk)


    def wait_special(g):
        @pl.when(k == 1)
        def _():
            wait_slot(g, 0)

        @pl.when((k == 0) & (r > 0))
        def _():
            wait_slot(g, 9)

    with scope("q1"):
        q_tile(1)
    with scope("own0"):
        step(0, [own], first=True)
    with scope("f_prev0"):
        f_prev(0, x >= 0)
    with scope("f_one0"):
        f_one(0, True)
    for c in w0:
        c.start()
    with scope("own1"):
        step(1, [own], first=True)
    with scope("tier_x"):

        @pl.when(tier_x)
        def _():
            @pl.when(jnp.logical_not(is_root))
            def _():
                s_x[0].wait_recv()

            s_y.start()

    with scope("wsp0"):
        wait_special(0)
    with scope("step0sp"):
        step(0, [special, prev_odd])
    with scope("f_prev1"):
        f_prev(1, x != 1)
    with scope("f_three0a"):
        f_three(0, x == 1)
    with scope("f_prev1b"):
        f_prev(1, x == 1)
    with scope("wsp1"):
        wait_special(1)
    with scope("step1sp"):
        step(1, [special, prev_odd])
    with scope("f_one0b"):
        f_one(0, False)
    with scope("f_three0"):
        f_three(0, x != 1)
    with scope("f_one1"):
        f_one(1, True)
    with scope("f_three1a"):
        f_three(1, x == 1)
    with scope("tier_y"):

        @pl.when(tier_y)
        def _():
            @pl.when(yl == 1)
            def _():
                s_y.wait_recv()

            for c in s_z:
                c.start()

    with scope("w0_1"):
        wait_slot(0, 2 + (1 - k))
    with scope("step0_1"):
        step(0, [slot(1, 0), slot(1, 1)])
    with scope("w0wait"):
        for c in w0:
            c.wait_recv()
    for c in w3a + w3b:
        c.start()
    w5[0].start()
    with scope("f_one1b"):
        f_one(1, False)
    with scope("w0_3"):
        wait_slot(0, 6 + (1 - k))
    with scope("step0_3"):
        step(0, [slot(3, 0), slot(3, 1)])
    with scope("tier_z"):

        @pl.when(tier_z)
        def _():
            @pl.when(z > 0)
            def _():
                s_z[0].wait_recv()

            s_k.start()

    with scope("f_two0"):
        f_two(0)
    with scope("w0_2"):
        wait_slot(0, 4 + (1 - k))
    last0 = [[slot(2, 0), slot(2, 1)]]
    with scope("pair0A"):
        pair_steps(0, 0, last0)
    with scope("tier_k"):

        @pl.when(k == 1)
        def _():
            s_k.wait_recv()

    with scope("finish0A"):
        finish(0, (0, 1))
    with scope("pair0B"):
        pair_steps(0, 2, last0)
    with scope("finish0B"):
        finish(0, (2, 3))
    with scope("f_three1b"):
        f_three(1, x != 1)
    with scope("w1_1"):
        wait_slot(1, 2 + (1 - k))
        wait_slot(1, 6 + (1 - k))
    with scope("step1b"):
        step(1, [slot(1, 0), slot(1, 1), slot(3, 0)])
    with scope("f_two1"):
        f_two(1)
    with scope("w3await"):
        for c in w3a:
            c.wait_recv()
    for c in w4:
        c.start()
    with scope("w1_2"):
        wait_slot(1, 4 + (1 - k))
    tail = [[slot(3, 1), slot(2, 0), slot(2, 1)]]
    with scope("pairA"):
        pair_steps(1, 4, tail)
    with scope("finishA"):
        finish(1, (0, 1))
    with scope("pairB"):
        pair_steps(1, 6, tail)
    with scope("finishB"):
        finish(1, (2, 3))
    with scope("w3bwait"):
        for c in w3b:
            c.wait_recv()
    w5[1].start()
    w5[2].start()
    with scope("w4wait"):
        for c in w4:
            c.wait_recv()
    w5[3].start()
    with scope("own_copy_wait"):
        own_copy.wait()
    NT_ = 512

    def two_heads(ref, pr):
        return jnp.concatenate([ref[2 * pr], ref[2 * pr + 1]], axis=1)

    def proj_own(n, c):
        cols = pl.ds(pl.multiple_of(n * NT_, NT_), NT_)
        y = None
        for pr in range(4):
            o = jnp.dot(two_heads(att_v, pr), wown_v[pr * 256 : pr * 256 + 256, cols], preferred_element_type=F32)
            y = o if y is None else y + o
        o0_v[:, cols] = y.astype(BF16)
        return c

    with scope("proj_own"):
        lax.fori_loop(0, 4, proj_own, 0)

    def wrows(pr, cols):
        return wpeer_v[pr * 256 : pr * 256 + 256, cols]

    with scope("w5wait"):
        for i in range(4):
            part = w_rows(((1 - k) * 4 + (z + (0, 1, 3, 2)[i]) % 4) * 8, 8)
            rcopy(part, part, wsend.at[6 + i], wrecv.at[6 + i], sib).wait_recv()
    with scope("att01wait"):
        for h in range(4):
            c_att(h).wait_recv()

    def proj_first(n, c):
        cols = pl.ds(pl.multiple_of(n * NT_, NT_), NT_)
        y = jnp.dot(two_heads(attp_v, 0), wrows(0, cols), preferred_element_type=F32)
        o1_v[:, cols] = y + jnp.dot(two_heads(attp_v, 1), wrows(1, cols), preferred_element_type=F32)
        return c

    with scope("proj_first"):
        lax.fori_loop(0, 4, proj_first, 0)
    with scope("att23wait"):
        for h in range(4, 8):
            c_att(h).wait_recv()

    def ocopy(n):
        cols = pl.ds(pl.multiple_of(n * NT_, NT_), NT_)
        return pltpu.make_async_copy(out_v.at[:, cols], out_hbm.at[:, cols], out_sem.at[n])

    def proj_last(n, c):
        cols = pl.ds(pl.multiple_of(n * NT_, NT_), NT_)
        y = jnp.dot(two_heads(attp_v, 2), wrows(2, cols), preferred_element_type=F32)
        y = y + jnp.dot(two_heads(attp_v, 3), wrows(3, cols), preferred_element_type=F32)
        y = (y + o1_v[:, cols]).astype(BF16).astype(F32)
        base = x_v[:, pl.ds(pl.multiple_of(j * 2048 + n * NT_, NT_), NT_)].astype(F32)
        out_v[:, cols] = (base + (o0_v[:, cols].astype(F32) + y)).astype(BF16)
        ocopy(n).start()
        return c

    with scope("proj_last"):
        lax.fori_loop(0, 4, proj_last, 0)

    for g in range(2):
        wait_sends(g)
    for c in w0 + w3a + w3b + w4 + w5:
        c.wait_send()

    @pl.when(is_root)
    def _():
        for c in s_x:
            c.wait_send()

    @pl.when(tier_x)
    def _():
        s_y.wait_send()

    @pl.when(tier_y)
    def _():
        for c in s_z:
            c.wait_send()

    @pl.when(tier_z)
    def _():
        s_k.wait_send()

    for h in range(8):
        c_att(h).wait_send()
    for n in range(4):
        ocopy(n).wait()


def local(tokens, norm_gain, w_query, w_key, w_value, w_out, window, sink_count, sink_bias):
    any_ = pl.BlockSpec(memory_space=pl.ANY)
    smem = pl.BlockSpec(memory_space=pltpu.SMEM)
    vmem = pl.BlockSpec(memory_space=pltpu.VMEM)
    dma = pltpu.SemaphoreType.DMA
    return pl.pallas_call(
        kernel,
        out_shape=jax.ShapeDtypeStruct((T, 2048), BF16),
        in_specs=[any_, vmem, any_, any_, any_, any_, smem, smem, smem],
        out_specs=any_,
        scratch_shapes=[
            pltpu.VMEM((T, D), BF16),
            pltpu.VMEM((T, D), BF16),
            pltpu.VMEM((D, 1024), BF16),
            pltpu.VMEM((D, 512), BF16),
            pltpu.VMEM((1024, 2048), BF16),
            pltpu.VMEM((1024, 2048), BF16),
            pltpu.VMEM((10, 2, T, 256), BF16),
            pltpu.VMEM((2, SROWS, 256), BF16),
            pltpu.VMEM((8, 256, T), BF16),
            pltpu.VMEM((8, VR, T), F32),
            pltpu.VMEM((8, 8, T), F32),
            pltpu.VMEM((T, T), jnp.int32),
            pltpu.VMEM((3 * T, T), F32),
            pltpu.VMEM((3 * T, T), F32),
            pltpu.VMEM((8, T, HD), BF16),
            pltpu.VMEM((8, T, HD), BF16),
            pltpu.VMEM((T, 2048), BF16),
            pltpu.VMEM((T, 2048), F32),
            pltpu.VMEM((T, 2048), BF16),
            dma((13,)),
            dma((2, N_HALO_SEND)),
            dma((2, 10)),
            dma((12,)),
            dma((12,)),
            dma((8,)),
            dma((4,)),
            dma((8,)),
            dma((8,)),
            dma((4,)),
        ],
        compiler_params=pltpu.CompilerParams(
            has_side_effects=True, collective_id=0, vmem_limit_bytes=64 * 1024 * 1024 - 65536
        ),
        name="block",
    )(tokens, norm_gain.reshape(1, D), w_query, w_key, w_value, w_out, window, sink_count, sink_bias)


def solution(mesh):
    in_specs = (
        P("seq", None),
        P(),
        P(None, "head"),
        P(None, "head"),
        P(None, "head"),
        P("head", None),
        P("head"),
        P("head"),
        P("head"),
    )
    return jax.shard_map(local, mesh=mesh, in_specs=in_specs, out_specs=P("seq", "head"), check_vma=False)
```

```python
import functools

import jax
import jax.numpy as jnp
from jax import lax
from jax.experimental import pallas as pl
from jax.experimental.pallas import tpu as pltpu
from jax.sharding import PartitionSpec as P

MESH = pl.DeviceIdType.MESH
HD = 128
T = 512
D = 4096
SINK = 4
SROWS = 16
EPS = 1e-05
scope = jax.named_scope
LOG2E = 1.4426950408889634
CSCALE = LOG2E * HD ** (-0.5)
NEG = -1e30
F32 = jnp.float32
BF16 = jnp.bfloat16
VR = 144

S_PREV, S_POS, S_NEG, S_FPOS, S_FNEG, S_D2D = 0, 1, 2, 3, 4, 5
N_HALO_SEND = S_D2D + 5


def kernel(
    x_hbm, gain_ref, wq_hbm, wk_hbm, wv_hbm, wo_hbm, win_ref, cnt_ref, bias_ref,
    out_hbm,
    x_v, n_v, wq_v, wkv_v, wown_v, wpeer_v, kv_v, sink_v, q_v, acc_v, m_v, rel_v, sa_v, sb_v,
    att_v, attp_v, o0_v, o1_v, out_v,
    in_sem, hsend, hrecv, wsend, wrecv, ssend, srecv, asend, arecv, out_sem,
):
    seq = lax.axis_index("seq")
    j = lax.axis_index("head")
    k = seq % 2
    x = (seq // 2) % 4
    r = seq // 8
    yl = r % 2
    z = r // 2
    peer = 1 - j

    def at(z_, yl_, x_, k_):
        return ((z_ * 2 + yl_) * 4 + x_) * 2 + k_

    sib = (at(z, yl, x, 1 - k), j)
    rn = (r + 1) % 8
    next_row = (rn * 8 + x * 2 + k, j)
    xp = (at(z, yl, (x + 1) % 4, k), j)
    xm = (at(z, yl, (x + 3) % 4, k), j)
    x2 = (at(z, yl, (x + 2) % 4, k), j)
    zp = (at((z + 1) % 4, yl, x, k), j)
    zm = (at((z + 3) % 4, yl, x, k), j)
    yo = (at(z, 1 - yl, x, k), j)
    head_peer = (seq, peer)
    diag = (at(z, 1 - yl, x, k), peer)

    def rcopy(src, dst, ss, rs, dev):
        return pltpu.make_async_remote_copy(
            src_ref=src, dst_ref=dst, send_sem=ss, recv_sem=rs, device_id=dev, device_id_type=MESH
        )

    def xcopy(i):
        rows = pl.ds(i * 128, 128)
        return pltpu.make_async_copy(x_hbm.at[rows], x_v.at[rows], in_sem.at[i])

    def kvcopy(i):
        g, w = i // 2, i % 2
        src = wk_hbm if w == 0 else wv_hbm
        return pltpu.make_async_copy(
            src.at[:, pl.ds(g * HD, HD)], wkv_v.at[:, pl.ds(i * HD, HD)], in_sem.at[4 + i]
        )

    def qcopy(i):
        cols = pl.ds(i * 256, 256)
        return pltpu.make_async_copy(wq_hbm.at[:, cols], wq_v.at[:, cols], in_sem.at[8 + i])

    own_copy = pltpu.make_async_copy(
        wo_hbm.at[:, pl.ds(pl.multiple_of(j * 2048, 2048), 2048)], wown_v, in_sem.at[12]
    )
    for i in range(4):
        xcopy(i).start()
    for i in range(4):
        kvcopy(i).start()
    for i in range(4):
        qcopy(i).start()
    own_copy.start()

    z2 = (at((z + 2) % 4, yl, x, k), j)
    prev_row = (((r + 7) % 8) * 8 + x * 2 + k, j)
    barrier = pltpu.get_barrier_semaphore()
    for dev in (sib, prev_row, xp, xm, x2, zp, zm, z2, yo, head_peer, diag):
        pl.semaphore_signal(barrier, inc=1, device_id=dev, device_id_type=MESH)

    L4 = ((k * 4 + z) * 2 + yl) * 4
    w_src = wo_hbm.at[
        pl.ds(pl.multiple_of(L4 * 16, 64), 64), pl.ds(pl.multiple_of(peer * 2048, 2048), 2048)
    ]
    w0 = [
        rcopy(w_src, wpeer_v.at[pl.ds(pl.multiple_of(L4 * 16, 64), 64)], wsend.at[i], wrecv.at[i], d)
        for i, d in enumerate((head_peer, diag))
    ]

    def w_rows(first, count):
        return wpeer_v.at[pl.ds(pl.multiple_of(first * 16, 64), count * 16)]

    L8 = (k * 4 + z) * 8
    eight = w_rows(L8, 8)
    own_lo, own_hi = w_rows(L8, 4), w_rows(L8 + 4, 4)
    w3a = [rcopy(own_lo, own_lo, wsend.at[2], wrecv.at[2], zp), rcopy(own_hi, own_hi, wsend.at[3], wrecv.at[3], zm)]
    w3b = [rcopy(own_hi, own_hi, wsend.at[10], wrecv.at[10], zp), rcopy(own_lo, own_lo, wsend.at[11], wrecv.at[11], zm)]
    Lm = (k * 4 + (z + 3) % 4) * 8
    Lp = (k * 4 + (z + 1) % 4) * 8
    lo4 = w_rows(Lm, 4)
    hi4 = w_rows(Lp + 4, 4)
    w4 = [rcopy(lo4, lo4, wsend.at[4], wrecv.at[4], zp), rcopy(hi4, hi4, wsend.at[5], wrecv.at[5], zm)]
    w5 = []
    for i in range(4):
        part = w_rows((k * 4 + (z + (0, 1, 3, 2)[i]) % 4) * 8, 8)
        w5.append(rcopy(part, part, wsend.at[6 + i], wrecv.at[6 + i], sib))

    own_slot = k
    prev_slot = 8 + k

    def slot_copy(src_slot, dst_slot, g, srow, dev, rslot):
        return rcopy(kv_v.at[src_slot, g], kv_v.at[dst_slot, g], hsend.at[g, srow], hrecv.at[g, rslot], dev)

    def c_prev(g):
        return slot_copy(own_slot, 8 + k, g, S_PREV, next_row, 8 + k)

    def c_pos(g, src):
        return slot_copy(src, 2 + k, g, S_POS, xp, 2 + k)

    def c_neg(g, src):
        return slot_copy(src, 6 + k, g, S_NEG, xm, 6 + k)

    def c_fpos(g):
        return slot_copy(2 + k, 4 + k, g, S_FPOS, xp, 4 + k)

    def c_fneg(g):
        return slot_copy(6 + k, 4 + k, g, S_FNEG, xm, 4 + k)

    def c_d2d(g, d):
        return slot_copy(2 * d + k, 2 * d + k, g, S_D2D + d, sib, 2 * d + k)

    def wait_slot(g, s):
        slot_copy(s, s, g, S_PREV, sib, s).wait_recv()

    def start_own(g):
        @pl.when(r < 7)
        def _():
            c_prev(g).start()

        @pl.when((x < 3) | (r == 0))
        def _():
            c_pos(g, own_slot).start()

        @pl.when((x == 0) | (r == 0))
        def _():
            c_neg(g, own_slot).start()

        @pl.when(k == 0)
        def _():
            c_d2d(g, 0).start()

    def f_prev(g, which):
        @pl.when((r > 0) & which)
        def _():
            wait_slot(g, 8 + k)

            @pl.when(x == 3)
            def _():
                c_pos(g, prev_slot).start()

            @pl.when(x > 0)
            def _():
                c_neg(g, prev_slot).start()

            @pl.when(k == 1)
            def _():
                c_d2d(g, 4).start()

    def f_one(g, early):
        @pl.when((x > 0) if early else (x == 0))
        def _():
            wait_slot(g, 2 + k)

            @pl.when(x < 3)
            def _():
                c_fpos(g).start()

            c_d2d(g, 1).start()

    def f_three(g, which):
        @pl.when(which)
        def _():
            wait_slot(g, 6 + k)

            @pl.when(x == 1)
            def _():
                c_fneg(g).start()

            c_d2d(g, 3).start()

    def f_two(g):
        wait_slot(g, 4 + k)
        c_d2d(g, 2).start()

    def wait_sends(g):
        @pl.when(r < 7)
        def _():
            c_prev(g).wait_send()

        c_pos(g, own_slot).wait_send()
        c_neg(g, own_slot).wait_send()

        @pl.when(x < 3)
        def _():
            c_fpos(g).wait_send()

        @pl.when(x == 1)
        def _():
            c_fneg(g).wait_send()

        @pl.when(k == 0)
        def _():
            c_d2d(g, 0).wait_send()

        @pl.when((k == 1) & (r > 0))
        def _():
            c_d2d(g, 4).wait_send()

        for d in (1, 2, 3):
            c_d2d(g, d).wait_send()

    sinks = sink_v.at[:]
    s_x = [rcopy(sinks, sinks, ssend.at[i], srecv.at[0], (at(0, 0, i + 1, 0), j)) for i in range(3)]
    s_y = rcopy(sinks, sinks, ssend.at[3], srecv.at[1], yo)
    s_z = [rcopy(sinks, sinks, ssend.at[4 + i], srecv.at[2], (at(i + 1, yl, x, 0), j)) for i in range(3)]
    s_k = rcopy(sinks, sinks, ssend.at[7], srecv.at[3], sib)
    is_root = seq == 0
    tier_x = (z == 0) & (yl == 0) & (k == 0)
    tier_y = (z == 0) & (k == 0)
    tier_z = k == 0

    def rel_rows(i, c):
        rows = pl.ds(i * 64, 64)
        a = lax.broadcasted_iota(jnp.int32, (64, T), 0) + i * 64
        b = lax.broadcasted_iota(jnp.int32, (64, T), 1)
        rel_v[rows, :] = b - a
        return c

    with scope("rel_rows"):
        lax.fori_loop(0, 8, rel_rows, 0)
    gain = gain_ref[...]

    def norm_rows(i, c):
        rows = pl.ds(i * 32, 32)
        xt = x_v[rows, :].astype(F32)
        ms = jnp.mean(xt * xt, axis=1, keepdims=True)
        n_v[rows, :] = (xt * lax.rsqrt(ms + EPS) * gain).astype(BF16)
        return c

    for i in range(4):
        with scope("xwait"):
            xcopy(i).wait()
        with scope("norm"):
            lax.fori_loop(i * 4, i * 4 + 4, norm_rows, 0)

    with scope("barrier"):
        pl.semaphore_wait(barrier, 11)

    with scope("kvwait"):
        for i in range(4):
            kvcopy(i).wait()
    with scope("kv"):
        y = jnp.dot(n_v[...], wkv_v[...], preferred_element_type=F32)
        for g in range(2):
            yg = y[:, g * 256 : g * 256 + 256]
            kv_v[own_slot, g, :, 0:HD] = yg[:, 0:HD].astype(BF16)
            for c in range(4):
                kv_v[own_slot, g, c * HD : c * HD + HD, HD : 2 * HD] = (
                    yg[c * HD : c * HD + HD, HD : 2 * HD].T.astype(BF16)
                )
            if g == 1:

                @pl.when(is_root)
                def _():
                    for e in range(2):
                        sink_v[e] = y[:SROWS, e * 256 : e * 256 + 256].astype(BF16)
                    for c in s_x:
                        c.start()

            start_own(g)
    def q_tile(i):
        qcopy(2 * i).wait()
        qcopy(2 * i + 1).wait()
        y = jnp.dot(n_v[...], wq_v[:, i * 512 : i * 512 + 512], preferred_element_type=F32)
        for h in range(4):
            qt = y[:, h * HD : h * HD + HD].astype(BF16).astype(F32).T * CSCALE
            hi = qt.astype(BF16)
            q_v[4 * i + h, 0:HD, :] = hi
            q_v[4 * i + h, HD : 2 * HD, :] = (qt - hi.astype(F32)).astype(BF16)

    with scope("q0"):
        q_tile(0)

    ones = jnp.ones((VR - HD, T), BF16)

    def values_t(slot, g):
        vt = [kv_v[slot, g, c * HD : c * HD + HD, HD : 2 * HD] for c in range(4)]
        return jnp.concatenate([jnp.concatenate(vt, axis=1), ones], axis=0)

    def scores(g, h, slots, first, s_ref):
        q = q_v[h]
        w = win_ref[h]
        top = None
        for b, (dist, place) in enumerate(slots):
            keys = kv_v[place, g, :, 0:HD]
            s = jnp.dot(jnp.concatenate([keys, keys], axis=1), q, preferred_element_type=F32)
            limit = jnp.where(seq >= dist, w - T * dist, -100000)
            rel = rel_v[...]
            seen = rel < limit
            if first:
                seen = seen & (rel >= 0)
            s = jnp.where(seen, s, NEG)
            s_ref[b * T : b * T + T, :] = s
            t = jnp.max(s, axis=0, keepdims=True)
            top = t if top is None else jnp.maximum(top, t)
        return top

    def weigh(g, h, slots, first, s_ref, top):
        if not first:
            old = m_v[h, 0:1, :]
            top = jnp.maximum(top, old)
        total = None
        for b, (_, place) in enumerate(slots):
            p = jnp.exp2(s_ref[b * T : b * T + T, :] - top).astype(BF16)
            o = jnp.dot(values_t(place, g), p, preferred_element_type=F32)
            total = o if total is None else total + o
        if not first:
            total = total + acc_v[h] * jnp.exp2(old - top)
        acc_v[h] = total
        m_v[h] = jnp.broadcast_to(top, (8, T))

    def step(g, slots, first=False, halfway=None):
        base = g * 4

        def body(i, top):
            if halfway is not None:

                @pl.when(i == 1)
                def _():
                    halfway()

            h = base + 2 * i
            top_b = scores(g, h + 1, slots, first, sb_v)
            weigh(g, h, slots, first, sa_v, top)
            top = scores(g, jnp.minimum(h + 2, base + 3), slots, first, sa_v)
            weigh(g, h + 1, slots, first, sb_v, top_b)
            return top

        lax.fori_loop(0, 2, body, scores(g, base, slots, first, sa_v))

    def c_att(h):
        return rcopy(att_v.at[h], attp_v.at[h], asend.at[h], arecv.at[h], head_peer)

    def finish_head(g, h):
        ks = sink_v[g, :, 0:HD]
        vt = sink_v[g, :, HD : 2 * HD].astype(F32).T.astype(BF16)
        s = jnp.dot(jnp.concatenate([ks, ks], axis=1), q_v[h], preferred_element_type=F32)
        s = s + bias_ref[h] * LOG2E
        row = lax.broadcasted_iota(jnp.int32, (SROWS, T), 0)
        pos = lax.broadcasted_iota(jnp.int32, (SROWS, T), 1) + seq * T
        is_open = (row < cnt_ref[h]) & (row < SINK) & (row <= pos - win_ref[h])
        s = jnp.where(is_open, s, NEG)
        old = m_v[h, 0:1, :]
        top = jnp.maximum(jnp.max(s, axis=0, keepdims=True), old)
        p = jnp.exp2(s - top)
        scale = jnp.exp2(old - top)
        total = acc_v[h, HD : HD + 1, :] * scale + jnp.sum(p, axis=0, keepdims=True)
        o = acc_v[h, 0:HD, :] * scale + jnp.dot(vt, p.astype(BF16), preferred_element_type=F32)
        return (o / total).T.astype(BF16)

    def finish(g, heads=(0, 1, 2, 3)):
        for i in heads:
            att_v[g * 4 + i] = finish_head(g, g * 4 + i)
            c_att(g * 4 + i).start()

    def pair_steps(g, h0, steps):
        items = [(slots, h0 + i) for slots in steps for i in range(2)]
        bufs = (sa_v, sb_v)
        last = None
        for n, (slots, h) in enumerate(items):
            top = scores(g, h, slots, False, bufs[n % 2])
            if last is not None:
                weigh(*last)
            last = (g, h, slots, False, bufs[n % 2], top)
        weigh(*last)

    own = (0, own_slot)
    special = (jnp.where(k == 0, 8, 1), jnp.where((k == 0) & (r > 0), 8, 0))
    prev_odd = (7 + k, jnp.where(r == 0, k, 9))

    def slot(d, kk):
        return (2 * d + k - kk, 2 * d + kk)


    def wait_special(g):
        @pl.when(k == 1)
        def _():
            wait_slot(g, 0)

        @pl.when((k == 0) & (r > 0))
        def _():
            wait_slot(g, 9)

    with scope("q1"):
        q_tile(1)
    with scope("own0"):
        step(0, [own], first=True)
    with scope("f_prev0"):
        f_prev(0, x >= 0)
    with scope("f_one0"):
        f_one(0, True)
    for c in w0:
        c.start()
    with scope("own1"):
        step(1, [own], first=True)
    with scope("tier_x"):

        @pl.when(tier_x)
        def _():
            @pl.when(jnp.logical_not(is_root))
            def _():
                s_x[0].wait_recv()

            s_y.start()

    with scope("wsp0"):
        wait_special(0)
    with scope("step0sp"):
        step(0, [special, prev_odd])
    with scope("f_prev1"):
        f_prev(1, x != 1)
    with scope("f_three0a"):
        f_three(0, x == 1)
    with scope("f_prev1b"):
        f_prev(1, x == 1)
    with scope("wsp1"):
        wait_special(1)
    with scope("step1sp"):
        step(1, [special, prev_odd])
    with scope("f_one0b"):
        f_one(0, False)
    with scope("f_three0"):
        f_three(0, x != 1)
    with scope("f_one1"):
        f_one(1, True)
    with scope("tier_y"):

        @pl.when(tier_y)
        def _():
            @pl.when(yl == 1)
            def _():
                s_y.wait_recv()

            for c in s_z:
                c.start()

    with scope("w0_1"):
        wait_slot(0, 2 + (1 - k))
    with scope("step0_1"):
        step(0, [slot(1, 0), slot(1, 1)])
    with scope("f_three1a"):
        f_three(1, x == 1)
    with scope("w0wait"):
        for c in w0:
            c.wait_recv()
    for c in w3a + w3b:
        c.start()
    w5[0].start()
    with scope("f_one1b"):
        f_one(1, False)
    with scope("w0_3"):
        wait_slot(0, 6 + (1 - k))
    with scope("step0_3"):
        step(0, [slot(3, 0), slot(3, 1)], halfway=lambda: f_two(0))
    with scope("tier_z"):

        @pl.when(tier_z)
        def _():
            @pl.when(z > 0)
            def _():
                s_z[0].wait_recv()

            s_k.start()

    with scope("w0_2"):
        wait_slot(0, 4 + (1 - k))
    last0 = [[slot(2, 0), slot(2, 1)]]
    with scope("pair0A"):
        pair_steps(0, 0, last0)
    with scope("tier_k"):

        @pl.when(k == 1)
        def _():
            s_k.wait_recv()

    with scope("finish0A"):
        finish(0, (0, 1))
    with scope("pair0B"):
        pair_steps(0, 2, last0)
    with scope("finish0B"):
        finish(0, (2, 3))
    with scope("f_three1b"):
        f_three(1, x != 1)
    with scope("w1_1"):
        wait_slot(1, 2 + (1 - k))
        wait_slot(1, 6 + (1 - k))
    with scope("step1b"):
        step(1, [slot(1, 0), slot(1, 1), slot(3, 0)], halfway=lambda: f_two(1))
    with scope("w3await"):
        for c in w3a:
            c.wait_recv()
    for c in w4:
        c.start()
    with scope("w1_2"):
        wait_slot(1, 4 + (1 - k))
    tail = [[slot(3, 1), slot(2, 0), slot(2, 1)]]
    with scope("pairA"):
        pair_steps(1, 4, tail)
    with scope("finishA"):
        finish(1, (0, 1))
    with scope("pairB"):
        pair_steps(1, 6, tail)
    with scope("finishB"):
        finish(1, (2, 3))
    with scope("w3bwait"):
        for c in w3b:
            c.wait_recv()
    w5[1].start()
    w5[2].start()
    with scope("w4wait"):
        for c in w4:
            c.wait_recv()
    w5[3].start()
    with scope("own_copy_wait"):
        own_copy.wait()
    NT_ = 512

    def two_heads(ref, pr):
        return jnp.concatenate([ref[2 * pr], ref[2 * pr + 1]], axis=1)

    def proj_own(n, c):
        cols = pl.ds(pl.multiple_of(n * NT_, NT_), NT_)
        y = None
        for pr in range(4):
            o = jnp.dot(two_heads(att_v, pr), wown_v[pr * 256 : pr * 256 + 256, cols], preferred_element_type=F32)
            y = o if y is None else y + o
        base = x_v[:, pl.ds(pl.multiple_of(j * 2048 + n * NT_, NT_), NT_)].astype(F32)
        o0_v[:, cols] = base + y.astype(BF16).astype(F32)
        return c

    with scope("proj_own"):
        lax.fori_loop(0, 4, proj_own, 0)

    def wrows(pr, cols):
        return wpeer_v[pr * 256 : pr * 256 + 256, cols]

    with scope("w5wait"):
        for i in range(4):
            part = w_rows(((1 - k) * 4 + (z + (0, 1, 3, 2)[i]) % 4) * 8, 8)
            rcopy(part, part, wsend.at[6 + i], wrecv.at[6 + i], sib).wait_recv()
    with scope("att01wait"):
        for h in range(4):
            c_att(h).wait_recv()

    def proj_first(n, c):
        cols = pl.ds(pl.multiple_of(n * NT_, NT_), NT_)
        y = jnp.dot(two_heads(attp_v, 0), wrows(0, cols), preferred_element_type=F32)
        o1_v[:, cols] = y + jnp.dot(two_heads(attp_v, 1), wrows(1, cols), preferred_element_type=F32)
        return c

    with scope("proj_first"):
        lax.fori_loop(0, 4, proj_first, 0)
    with scope("att45wait"):
        for h in range(4, 6):
            c_att(h).wait_recv()

    def proj_mid(n, c):
        cols = pl.ds(pl.multiple_of(n * NT_, NT_), NT_)
        y = jnp.dot(two_heads(attp_v, 2), wrows(2, cols), preferred_element_type=F32)
        o1_v[:, cols] = o1_v[:, cols] + y
        return c

    with scope("proj_mid"):
        lax.fori_loop(0, 4, proj_mid, 0)
    with scope("att67wait"):
        for h in range(6, 8):
            c_att(h).wait_recv()

    def ocopy(n):
        cols = pl.ds(pl.multiple_of(n * NT_, NT_), NT_)
        return pltpu.make_async_copy(out_v.at[:, cols], out_hbm.at[:, cols], out_sem.at[n])

    def proj_last(n, c):
        cols = pl.ds(pl.multiple_of(n * NT_, NT_), NT_)
        y = jnp.dot(two_heads(attp_v, 3), wrows(3, cols), preferred_element_type=F32)
        y = (y + o1_v[:, cols]).astype(BF16).astype(F32)
        out_v[:, cols] = (o0_v[:, cols] + y).astype(BF16)
        ocopy(n).start()
        return c

    with scope("proj_last"):
        lax.fori_loop(0, 4, proj_last, 0)

    for g in range(2):
        wait_sends(g)
    for c in w0 + w3a + w3b + w4 + w5:
        c.wait_send()

    @pl.when(is_root)
    def _():
        for c in s_x:
            c.wait_send()

    @pl.when(tier_x)
    def _():
        s_y.wait_send()

    @pl.when(tier_y)
    def _():
        for c in s_z:
            c.wait_send()

    @pl.when(tier_z)
    def _():
        s_k.wait_send()

    for h in range(8):
        c_att(h).wait_send()
    for n in range(4):
        ocopy(n).wait()


def local(tokens, norm_gain, w_query, w_key, w_value, w_out, window, sink_count, sink_bias):
    any_ = pl.BlockSpec(memory_space=pl.ANY)
    smem = pl.BlockSpec(memory_space=pltpu.SMEM)
    vmem = pl.BlockSpec(memory_space=pltpu.VMEM)
    dma = pltpu.SemaphoreType.DMA
    return pl.pallas_call(
        kernel,
        out_shape=jax.ShapeDtypeStruct((T, 2048), BF16),
        in_specs=[any_, vmem, any_, any_, any_, any_, smem, smem, smem],
        out_specs=any_,
        scratch_shapes=[
            pltpu.VMEM((T, D), BF16),
            pltpu.VMEM((T, D), BF16),
            pltpu.VMEM((D, 1024), BF16),
            pltpu.VMEM((D, 512), BF16),
            pltpu.VMEM((1024, 2048), BF16),
            pltpu.VMEM((1024, 2048), BF16),
            pltpu.VMEM((10, 2, T, 256), BF16),
            pltpu.VMEM((2, SROWS, 256), BF16),
            pltpu.VMEM((8, 256, T), BF16),
            pltpu.VMEM((8, VR, T), F32),
            pltpu.VMEM((8, 8, T), F32),
            pltpu.VMEM((T, T), jnp.int32),
            pltpu.VMEM((3 * T, T), F32),
            pltpu.VMEM((3 * T, T), F32),
            pltpu.VMEM((8, T, HD), BF16),
            pltpu.VMEM((8, T, HD), BF16),
            pltpu.VMEM((T, 2048), F32),
            pltpu.VMEM((T, 2048), F32),
            pltpu.VMEM((T, 2048), BF16),
            dma((13,)),
            dma((2, N_HALO_SEND)),
            dma((2, 10)),
            dma((12,)),
            dma((12,)),
            dma((8,)),
            dma((4,)),
            dma((8,)),
            dma((8,)),
            dma((4,)),
        ],
        compiler_params=pltpu.CompilerParams(
            has_side_effects=True, collective_id=0, vmem_limit_bytes=64 * 1024 * 1024 - 65536
        ),
        name="block",
    )(tokens, norm_gain.reshape(1, D), w_query, w_key, w_value, w_out, window, sink_count, sink_bias)


def solution(mesh):
    in_specs = (
        P("seq", None),
        P(),
        P(None, "head"),
        P(None, "head"),
        P(None, "head"),
        P("head", None),
        P("head"),
        P("head"),
        P("head"),
    )
    return jax.shard_map(local, mesh=mesh, in_specs=in_specs, out_specs=P("seq", "head"), check_vma=False)
```
